32 devices in a mesh: dp: 8 (over y, x, core), tensor: 4 (over z).
Axes of the slice: x: 2, y: 2, z: 4, core: 2. Of those that a mesh axis runs over, the one named last changes fastest.
Arguments:
- block_in: bfloat16 [16384, 2048], P(('dp', 'tensor')), may hold values from -6 to 6
- ln_gain: float32 [2048], replicated, may hold values from 0.5 to 1.5
- ln_bias: float32 [2048], replicated, may hold values from -3 to 3
- qkv_weight: bfloat16 [3, 2048, 2048], P(None, None, 'tensor'), may hold values from -1 to 1
- qkv_bias: float32 [3, 2048], P(None, 'tensor'), may hold values from -3 to 3
- out_weight: bfloat16 [2048, 2048], P('tensor'), may hold values from -0.5 to 0.5
- out_bias: float32 [2048], replicated, may hold values from -3 to 3
- up_weight: bfloat16 [2048, 8192], P(None, 'tensor'), may hold values from -0.125 to 0.125
- up_bias: float32 [8192], P('tensor'), may hold values from -3 to 3
- down_weight: bfloat16 [8192, 2048], P('tensor'), may hold values from -0.0625 to 0.0625
- down_bias: float32 [2048], replicated, may hold values from -3 to 3
- segments: int32 [16384], P('dp'), may hold values from 0 to 3, as said below
- cotangent: bfloat16 [16384, 2048], P(('dp', 'tensor')), may hold values from -6 to 6
Outputs:
- block_out: bfloat16 [16384, 2048], P(('dp', 'tensor'))
- input_grad: bfloat16 [16384, 2048], P(('dp', 'tensor'))
- ln_gain_grad: float32 [2048], replicated
- ln_bias_grad: float32 [2048], replicated
- qkv_weight_grad: float32 [3, 2048, 2048], P(None, 'dp', 'tensor')
- qkv_bias_grad: float32 [3, 2048], P(None, 'tensor')
- out_weight_grad: float32 [2048, 2048], P('tensor', 'dp')
- out_bias_grad: float32 [2048], replicated
- up_weight_grad: float32 [2048, 8192], P('dp', 'tensor')
- up_bias_grad: float32 [8192], P('tensor')
- down_weight_grad: float32 [8192, 2048], P('tensor', 'dp')
- down_bias_grad: float32 [2048], replicated
The draws below stay inside these ranges and needn't reach their ends.
Inputs may be any that keep to these rules, and one draw needn't show every extreme that they name: `segments`: along each sequence of 2048 tokens the segment numbers start at 0, never fall, and rise by one at each of three document starts.
All inputs are finite; a program needn't handle non-finite values.
Results may differ from the reference program's by a relative error of at most 0.012.
Values may be sent and summed in bfloat16 or wider, within the bound.
A program may use at most 320 MiB of HBM per device.

```python
import jax
import jax.numpy as jnp
from jax import lax

D = 2048
H = 32
HD = 64
ROT = 32
FF = 8192
SEQ = 2048
TOKENS = 16384
N_TENSOR = 4


def draw_qkv_weight(key, part):
    spread = D ** (-0.5)
    base = jax.random.normal(jax.random.fold_in(key, 11), (3, D, D), jnp.float32) * spread
    return jnp.clip(base, -1.0, 1.0).astype(jnp.bfloat16)


def draw_segments(key, part):
    count = TOKENS // SEQ
    least = SEQ // 10
    room = SEQ - 4 * least + 1
    picks = jnp.sort(jax.random.randint(jax.random.fold_in(key, 21), (count, 3), 0, room, dtype=jnp.int32), axis=1)
    cuts = picks + least * jnp.arange(1, 4, dtype=jnp.int32)[None, :]
    place = jnp.arange(SEQ, dtype=jnp.int32)
    ids = jnp.sum((place[None, :, None] >= cuts[:, None, :]).astype(jnp.int32), axis=-1)
    return ids.reshape(TOKENS).astype(jnp.int32)


def spiked(entries, stream_key, source, target, shards_of, factor):
    owner, partner = [(jnp.arange(entries.shape[position]) // (entries.shape[position] // shards_of)).reshape([-1 if axis == position else 1 for axis in range(entries.ndim)]) for position in (source, target)]
    chosen = jax.random.permutation(stream_key, shards_of)[partner]
    strong = (owner == chosen) | (owner == (partner + shards_of // 2) % shards_of)
    return jnp.where(strong, factor * entries, entries)


def levels(own_key, extent, cuts, low, top_value):
    loudness, own = 1.0, jax.random.fold_in(own_key, 6)
    for dim, blocks in cuts:
        heights = jnp.exp(jax.random.uniform(jax.random.fold_in(own, dim), (blocks,), jnp.float32, low / len(cuts), top_value / len(cuts)))
        loudness = loudness * jnp.repeat(heights, extent[dim] // blocks).reshape([-1 if axis == dim else 1 for axis in range(len(extent))])
    return loudness


def normal_values(stream_key, extent, scale, most, shards=(), held_as=jnp.bfloat16):
    array = jax.random.normal(stream_key, extent, jnp.float32) * scale
    if len(shards) > 0:
        array = levels(stream_key, extent, shards, -0.22, 0.18) * array
    return jnp.clip(array, min=-most, max=most).astype(held_as)


def gaussian_with(key, shape, width, most, pieces, heavy, held_as=jnp.bfloat16):
    values = width * jax.random.normal(key, shape, jnp.float32)
    if pieces:
        values = values * levels(key, shape, pieces, -0.22, 0.18)
    return jnp.clip(spiked(values, jax.random.fold_in(key, 3), *heavy), -most, most).astype(held_as)


def setup_inputs(seed: int = 0) -> dict:
    key_of = jax.random.split(jax.random.key(seed), 14)
    block_in = normal_values(key_of[0], (TOKENS, D), 1.0, 6.0, ((0, 32),))
    ln_gain = jnp.clip(1.0 + 0.1 * jax.random.normal(key_of[1], (D,), jnp.float32), 0.5, 1.5)
    ln_bias = normal_values(key_of[2], (D,), 0.5, 3.0, (), jnp.float32)
    qkv_weight = draw_qkv_weight(jax.random.fold_in(key_of[13], 71), 0)
    qkv_bias = normal_values(key_of[4], (3, D), 0.5, 3.0, ((1, 4),), jnp.float32)
    out_weight = normal_values(key_of[5], (D, D), (D // 16) ** -0.5, 0.5, ((0, 4),))
    out_bias = normal_values(key_of[6], (D,), 0.5, 3.0, (), jnp.float32)
    up_weight = normal_values(key_of[7], (D, FF), D ** -0.5, 0.125, ((1, 4),))
    up_bias = normal_values(key_of[8], (FF,), 0.5, 3.0, ((0, 4),), jnp.float32)
    down_weight = normal_values(key_of[9], (FF, D), FF ** -0.5, 0.0625, ((0, 4),))
    down_bias = normal_values(key_of[10], (D,), 0.5, 3.0, (), jnp.float32)
    segments = draw_segments(jax.random.fold_in(key_of[13], 71), 0)
    cotangent = gaussian_with(key_of[12], (TOKENS, D), 1.0, 6.0, ((0, 32),), (0, 1, 32, 2.75))
    return {"block_in": block_in, "ln_gain": ln_gain, "ln_bias": ln_bias, "qkv_weight": qkv_weight, "qkv_bias": qkv_bias, "out_weight": out_weight, "out_bias": out_bias, "up_weight": up_weight, "up_bias": up_bias, "down_weight": down_weight, "down_bias": down_bias, "segments": segments, "cotangent": cotangent}


EPSILON = 1e-05
NEGATIVE = -1e+30
ROOT_TWO_PI = 0.7978845608028654

def normalize(rows):
    wide = rows.astype(jnp.float32)
    centre = wide - lax.optimization_barrier(jnp.mean(wide, axis=-1, keepdims=True))
    inv_scale = lax.rsqrt(lax.optimization_barrier(jnp.mean(centre * centre, axis=-1, keepdims=True)) + EPSILON)
    return (centre * inv_scale, inv_scale)

def gelu_pair(pre):
    inner = ROOT_TWO_PI * (pre + 0.044715 * pre * pre * pre)
    tangent = jnp.tanh(inner)
    value = 0.5 * pre * (1.0 + tangent)
    slope = 0.5 * (1.0 + tangent) + 0.5 * pre * (1.0 - tangent * tangent) * ROOT_TWO_PI * (1.0 + 3.0 * 0.044715 * pre * pre)
    return (value, slope)

def rotary_tables(segments, rotary):
    length = segments.shape[0]
    index = jnp.arange(length, dtype=jnp.int32)
    first = jnp.concatenate([jnp.ones((1,), jnp.bool_), segments[1:] != segments[:-1]])
    starts = lax.cummax(jnp.where(first, index, jnp.zeros_like(index)), axis=0)
    place = (index - starts).astype(jnp.float32)
    freq = 10000.0 ** (-(2.0 * jnp.arange(rotary // 2, dtype=jnp.float32)) / rotary)
    angle = place[:, None] * freq[None, :]
    return (jnp.cos(angle), jnp.sin(angle))

def rotate(values, cosine, sine, rotary):
    half = rotary // 2
    first = values[..., :half]
    second = values[..., half:rotary]
    cosine = cosine[:, None, :]
    sine = sine[:, None, :]
    return jnp.concatenate([first * cosine - second * sine, second * cosine + first * sine, values[..., rotary:]], axis=-1)

def unrotate(grads, cosine, sine, rotary):
    half = rotary // 2
    first = grads[..., :half]
    second = grads[..., half:rotary]
    cosine = cosine[:, None, :]
    sine = sine[:, None, :]
    return jnp.concatenate([first * cosine + second * sine, second * cosine - first * sine, grads[..., rotary:]], axis=-1)

def head_forward(query, key, value, allowed):
    scores = jnp.dot(query, key.T, preferred_element_type=jnp.float32) * HD ** (-0.5)
    scores = jnp.where(allowed, scores, NEGATIVE)
    peak = lax.optimization_barrier(jnp.max(scores, axis=-1, keepdims=True))
    total = peak + jnp.log(lax.optimization_barrier(jnp.sum(jnp.exp(scores - peak), axis=-1, keepdims=True)))
    probs = jnp.exp(scores - total).astype(jnp.bfloat16)
    result = jnp.dot(probs, value, preferred_element_type=jnp.float32).astype(jnp.bfloat16)
    return (result, total[:, 0])

def head_backward(query, key, value, result, result_grad, total, allowed):
    scores = jnp.dot(query, key.T, preferred_element_type=jnp.float32) * HD ** (-0.5)
    scores = jnp.where(allowed, scores, NEGATIVE)
    probs_f = jnp.exp(scores - total[:, None])
    probs = probs_f.astype(jnp.bfloat16)
    value_grad = jnp.dot(probs.T, result_grad, preferred_element_type=jnp.float32)
    probs_grad = jnp.dot(result_grad, value.T, preferred_element_type=jnp.float32)
    delta = lax.optimization_barrier(jnp.sum(result_grad.astype(jnp.float32) * result.astype(jnp.float32), axis=-1))
    score_grad = (probs_f * (probs_grad - delta[:, None]) * HD ** (-0.5)).astype(jnp.bfloat16)
    query_grad = jnp.dot(score_grad, key, preferred_element_type=jnp.float32)
    key_grad = jnp.dot(score_grad.T, query, preferred_element_type=jnp.float32)
    return (query_grad, key_grad, value_grad)

def heads_first(values):
    return jnp.transpose(values, (1, 0, 2))

def reference(block_in, ln_gain, ln_bias, qkv_weight, qkv_bias, out_weight, out_bias, up_weight, up_bias, down_weight, down_bias, segments, cotangent):
    count = TOKENS // SEQ
    col_block = D // N_TENSOR
    ff_block = FF // N_TENSOR
    inputs = (block_in.reshape(count, SEQ, D), segments.reshape(count, SEQ), cotangent.reshape(count, SEQ, D))

    def one_sequence(carry, item):
        rows, seg, grad_out = item
        normed, inv_scale = normalize(rows)
        hidden = (normed * ln_gain + ln_bias).astype(jnp.bfloat16)
        cosine, sine = rotary_tables(seg, ROT)
        projected = jnp.stack([jnp.dot(hidden, qkv_weight[part], preferred_element_type=jnp.float32) for part in range(3)]) + qkv_bias[:, None, :]
        query = rotate(projected[0].reshape(SEQ, H, HD), cosine, sine, ROT).astype(jnp.bfloat16)
        key = rotate(projected[1].reshape(SEQ, H, HD), cosine, sine, ROT).astype(jnp.bfloat16)
        value = projected[2].reshape(SEQ, H, HD).astype(jnp.bfloat16)
        index = jnp.arange(SEQ, dtype=jnp.int32)
        allowed = (index[None, :] <= index[:, None]) & (seg[None, :] == seg[:, None])

        def forward_head(operands):
            return head_forward(operands[0], operands[1], operands[2], allowed)
        results, totals = lax.map(forward_head, (heads_first(query), heads_first(key), heads_first(value)))
        attended = heads_first(results).reshape(SEQ, D)
        act_pre = jnp.dot(hidden, up_weight, preferred_element_type=jnp.float32) + up_bias
        act_value, act_slope = gelu_pair(act_pre)
        act = act_value.astype(jnp.bfloat16)
        branch = jnp.zeros((SEQ, D), jnp.float32)
        for block in range(N_TENSOR):
            cols = slice(block * col_block, (block + 1) * col_block)
            units = slice(block * ff_block, (block + 1) * ff_block)
            piece = jnp.dot(attended[:, cols], out_weight[cols], preferred_element_type=jnp.float32) + jnp.dot(act[:, units], down_weight[units], preferred_element_type=jnp.float32)
            branch = branch + piece.astype(jnp.bfloat16).astype(jnp.float32)
        block_out = (rows.astype(jnp.float32) + branch + out_bias + down_bias).astype(jnp.bfloat16)
        bias_sum = lax.optimization_barrier(jnp.sum(grad_out.astype(jnp.float32), axis=0))
        down_grad = jnp.dot(act.T, grad_out, preferred_element_type=jnp.float32)
        out_grad = jnp.dot(attended.T, grad_out, preferred_element_type=jnp.float32)
        act_grad = jnp.dot(grad_out, down_weight.T, preferred_element_type=jnp.float32) * act_slope
        up_bias_grad = lax.optimization_barrier(jnp.sum(act_grad, axis=0))
        act_grad_b = act_grad.astype(jnp.bfloat16)
        up_grad = jnp.dot(hidden.T, act_grad_b, preferred_element_type=jnp.float32)
        attended_grad = jnp.dot(grad_out, out_weight.T, preferred_element_type=jnp.float32).astype(jnp.bfloat16).reshape(SEQ, H, HD)

        def backward_head(operands):
            return head_backward(operands[0], operands[1], operands[2], operands[3], operands[4], operands[5], allowed)
        query_grad, key_grad, value_grad = lax.map(backward_head, (heads_first(query), heads_first(key), heads_first(value), results, heads_first(attended_grad), totals))
        query_grad = unrotate(heads_first(query_grad), cosine, sine, ROT).reshape(SEQ, D)
        key_grad = unrotate(heads_first(key_grad), cosine, sine, ROT).reshape(SEQ, D)
        value_grad = heads_first(value_grad).reshape(SEQ, D)
        projected_grad = jnp.stack([query_grad, key_grad, value_grad])
        qkv_bias_grad = lax.optimization_barrier(jnp.sum(projected_grad, axis=1))
        projected_grad_b = projected_grad.astype(jnp.bfloat16)
        qkv_grad = jnp.stack([jnp.dot(hidden.T, projected_grad_b[part], preferred_element_type=jnp.float32) for part in range(3)])
        hidden_grad = jnp.zeros((SEQ, D), jnp.float32)
        for block in range(N_TENSOR):
            cols = slice(block * col_block, (block + 1) * col_block)
            units = slice(block * ff_block, (block + 1) * ff_block)
            piece = jnp.dot(act_grad_b[:, units], up_weight[:, units].T, preferred_element_type=jnp.float32)
            for part in range(3):
                piece = piece + jnp.dot(projected_grad_b[part][:, cols], qkv_weight[part][:, cols].T, preferred_element_type=jnp.float32)
            hidden_grad = hidden_grad + piece.astype(jnp.bfloat16).astype(jnp.float32)
        gain_grad = lax.optimization_barrier(jnp.sum(hidden_grad * normed, axis=0))
        shift_grad = lax.optimization_barrier(jnp.sum(hidden_grad, axis=0))
        scaled = hidden_grad * ln_gain
        inner = scaled - lax.optimization_barrier(jnp.mean(scaled, axis=-1, keepdims=True)) - normed * lax.optimization_barrier(jnp.mean(scaled * normed, axis=-1, keepdims=True))
        input_grad = (grad_out.astype(jnp.float32) + inv_scale * inner).astype(jnp.bfloat16)
        updates = (gain_grad, shift_grad, qkv_grad, qkv_bias_grad, out_grad, bias_sum, up_grad, up_bias_grad, down_grad)
        carry = tuple((total + extra for total, extra in zip(carry, updates)))
        return (carry, (block_out, input_grad))
    start = (jnp.zeros((D,), jnp.float32), jnp.zeros((D,), jnp.float32), jnp.zeros((3, D, D), jnp.float32), jnp.zeros((3, D), jnp.float32), jnp.zeros((D, D), jnp.float32), jnp.zeros((D,), jnp.float32), jnp.zeros((D, FF), jnp.float32), jnp.zeros((FF,), jnp.float32), jnp.zeros((FF, D), jnp.float32))
    sums, (outputs, in_grads) = lax.scan(one_sequence, start, inputs)
    gain_grad, shift_grad, qkv_grad, qkv_bias_grad, out_grad, bias_sum, up_grad, up_bias_grad, down_grad = sums
    return (outputs.reshape(TOKENS, D), in_grads.reshape(TOKENS, D), gain_grad, shift_grad, qkv_grad, qkv_bias_grad, out_grad, bias_sum, up_grad, up_bias_grad, down_grad, bias_sum)
```

```python
import functools

import jax
import jax.numpy as jnp
from jax import lax
from jax.experimental import pallas as pl
from jax.experimental.pallas import tpu as pltpu
from jax.sharding import PartitionSpec as P

HD = 64
ROT = 32

EPSILON = 1e-05
NEGATIVE = -1e30
ROOT_TWO_PI = 0.7978845608028654
MESH = pl.DeviceIdType.MESH


def normalize(rows):
    wide = rows.astype(jnp.float32)
    centre = wide - jnp.mean(wide, axis=-1, keepdims=True)
    inv_scale = lax.rsqrt(jnp.mean(centre * centre, axis=-1, keepdims=True) + EPSILON)
    return (centre * inv_scale, inv_scale)


def gelu_pair(pre):
    inner = ROOT_TWO_PI * (pre + 0.044715 * pre * pre * pre)
    tangent = jnp.tanh(inner)
    value = 0.5 * pre * (1.0 + tangent)
    slope = 0.5 * (1.0 + tangent) + 0.5 * pre * (1.0 - tangent * tangent) * ROOT_TWO_PI * (
        1.0 + 3.0 * 0.044715 * pre * pre
    )
    return (value, slope)


def sum_kernel(axes, x_ref, out_ref, *scratch):
    barrier = pltpu.get_barrier_semaphore()
    peers = 0
    for name, size in axes:
        me = lax.axis_index(name)
        for step in range(1, size):
            pl.semaphore_signal(
                barrier, inc=1, device_id={name: lax.rem(me + step, size)}, device_id_type=MESH
            )
            peers += 1
    pl.semaphore_wait(barrier, peers)
    held = x_ref
    for number, (name, size) in enumerate(axes):
        slots, total, send, receive = scratch[4 * number : 4 * number + 4]
        me = lax.axis_index(name)
        copies = []
        for step in range(1, size):
            copy = pltpu.make_async_remote_copy(
                src_ref=held,
                dst_ref=slots.at[step - 1],
                send_sem=send.at[step - 1],
                recv_sem=receive.at[step - 1],
                device_id={name: lax.rem(me + step, size)},
                device_id_type=MESH,
            )
            copy.start()
            copies.append(copy)
        for copy in copies:
            copy.wait()
        made = jnp.zeros(x_ref.shape, jnp.float32)
        for device in range(size):
            piece = jnp.where(me == device, held[...], 0.0)
            for step in range(1, size):
                piece = piece + jnp.where(
                    lax.rem(me + size - step, size) == device, slots[step - 1], 0.0
                )
            made = made + piece
        total[...] = made
        held = total
    out_ref[...] = held[...]


def small_sum(values, axes, collective_id):
    scratch = []
    for _, size in axes:
        scratch += [
            pltpu.VMEM((size - 1, *values.shape), jnp.float32),
            pltpu.VMEM(values.shape, jnp.float32),
            pltpu.SemaphoreType.DMA((size - 1,)),
            pltpu.SemaphoreType.DMA((size - 1,)),
        ]
    return pl.pallas_call(
        functools.partial(sum_kernel, axes),
        out_shape=jax.ShapeDtypeStruct(values.shape, jnp.float32),
        in_specs=[pl.BlockSpec(memory_space=pltpu.VMEM)],
        out_specs=pl.BlockSpec(memory_space=pltpu.VMEM),
        scratch_shapes=scratch,
        compiler_params=pltpu.CompilerParams(collective_id=collective_id, has_side_effects=True),
        name="small_sum",
    )(values)


def lanes_of(*parts):
    return jnp.concatenate([part.reshape(-1, 128) for part in parts], axis=0)


LOG2E = 1.4426950408889634
BLOCK = 256


def attention_bounds(segments):
    length = segments.shape[0]
    begins = jnp.sum(
        (segments[None, :] < jnp.arange(1, 4, dtype=jnp.int32)[:, None]).astype(jnp.int32), axis=1
    )
    start = jnp.zeros_like(segments)
    for number in range(1, 4):
        start = jnp.where(segments == number, begins[number - 1], start)
    blocks = length // BLOCK
    rows = start.reshape(blocks, BLOCK)
    low, high = rows[:, 0], rows[:, BLOCK - 1]
    index = jnp.arange(blocks, dtype=jnp.int32)
    key_first = low // BLOCK
    key_whole = jnp.minimum((high + BLOCK - 1) // BLOCK, index)
    later = index[None, :] > index[:, None]
    query_whole = index + 1 + jnp.sum(
        (later & (high[None, :] <= index[:, None] * BLOCK)).astype(jnp.int32), axis=1
    )
    query_last = index + 1 + jnp.sum(
        (later & (low[None, :] < (index[:, None] + 1) * BLOCK)).astype(jnp.int32), axis=1
    )
    return start, jnp.stack([key_first, key_whole, query_whole, query_last])


def head_rows(values, head):
    row = lax.broadcasted_iota(jnp.int32, values.shape, 0)
    return jnp.where(row // HD == head, values, jnp.zeros_like(values))


def head_lanes(values, head):
    lane = lax.broadcasted_iota(jnp.int32, values.shape, 1)
    return jnp.where(lane // HD == head, values, jnp.zeros_like(values))


def allowed_tile(start_row, key_block, query_block):
    shape = (BLOCK, BLOCK)
    key_index = key_block * BLOCK + lax.broadcasted_iota(jnp.int32, shape, 0)
    query_index = query_block * BLOCK + lax.broadcasted_iota(jnp.int32, shape, 1)
    return (key_index <= query_index) & (key_index >= start_row)


def forward_kernel(bounds, start_ref, q_ref, k_ref, v_ref, out_ref, lse_ref, vt_ref):
    i = pl.program_id(1)
    blocks = k_ref.shape[0] // BLOCK

    @pl.when(i == 0)
    def _():
        for b in range(blocks):
            vt_ref[:, b * BLOCK : (b + 1) * BLOCK] = v_ref[b * BLOCK : (b + 1) * BLOCK, :].T

    query = q_ref[...].T
    queries = [head_rows(query, head) for head in range(2)]
    start_row = start_ref[...]

    def step(masked):
        def body(j, carry):
            at = pl.ds(pl.multiple_of(j * BLOCK, BLOCK), BLOCK)
            key = k_ref[at, :]
            new = []
            if masked:
                allowed = allowed_tile(start_row, j, i)
            for head in range(2):
                peak, total, acc = carry[head]
                scores = jnp.dot(key, queries[head], preferred_element_type=jnp.float32)
                scores = scores * (HD**-0.5 * LOG2E)
                if masked:
                    scores = jnp.where(allowed, scores, NEGATIVE)
                top = jnp.maximum(peak, jnp.max(scores, axis=0, keepdims=True))
                probs = jnp.exp2(scores - top)
                shrink = jnp.exp2(peak - top)
                total = total * shrink + jnp.sum(probs, axis=0, keepdims=True)
                acc = acc * shrink + jnp.dot(
                    vt_ref[head * HD : (head + 1) * HD, at],
                    probs.astype(jnp.bfloat16),
                    preferred_element_type=jnp.float32,
                )
                new.append((top, total, acc))
            return tuple(new)

        return body

    carry = tuple(
        (
            jnp.full((1, BLOCK), NEGATIVE, jnp.float32),
            jnp.zeros((1, BLOCK), jnp.float32),
            jnp.zeros((HD, BLOCK), jnp.float32),
        )
        for _ in range(2)
    )
    first, whole = bounds[0, i], bounds[1, i]
    carry = lax.fori_loop(first, whole, step(True), carry)
    carry = lax.fori_loop(jnp.maximum(whole, first), i, step(False), carry)
    carry = step(True)(i, carry)
    rows = [acc / total for _, total, acc in carry]
    out_ref[...] = jnp.concatenate(rows, axis=0).T.astype(jnp.bfloat16)
    lse_ref[0] = jnp.concatenate([top + jnp.log2(total) for top, total, _ in carry], axis=0)


def attention_forward(bounds, start, query, key, value):
    length, cols = query.shape
    pairs, blocks = cols // (2 * HD), length // BLOCK
    width = 2 * HD
    whole = pl.BlockSpec((length, width), lambda p, i, b: (0, p))
    block = pl.BlockSpec((BLOCK, width), lambda p, i, b: (i, p))
    return pl.pallas_call(
        forward_kernel,
        out_shape=(
            jax.ShapeDtypeStruct((length, cols), jnp.bfloat16),
            jax.ShapeDtypeStruct((pairs, 2, length), jnp.float32),
        ),
        grid_spec=pltpu.PrefetchScalarGridSpec(
            num_scalar_prefetch=1,
            grid=(pairs, blocks),
            in_specs=[pl.BlockSpec((1, BLOCK), lambda p, i, b: (0, i)), block, whole, whole],
            out_specs=(block, pl.BlockSpec((1, 2, BLOCK), lambda p, i, b: (p, 0, i))),
            scratch_shapes=[pltpu.VMEM((width, length), jnp.bfloat16)],
        ),
        compiler_params=pltpu.CompilerParams(dimension_semantics=("arbitrary", "arbitrary")),
        cost_estimate=pl.CostEstimate(
            flops=16 * 10**9, bytes_accessed=4 * 2 * length * cols, transcendentals=0
        ),
        name="attention_forward",
    )(bounds, start.reshape(1, length), query, key, value)


def turn(values, cosine, sine, sign):
    lane = lax.broadcasted_iota(jnp.int32, values.shape, 1)
    half = ROT // 2
    right = pltpu.roll(values, half, 1)
    left = pltpu.roll(values, values.shape[1] - half, 1)
    mixed = jnp.where(lane % HD < half, -left, right)
    return values * cosine + (sign * mixed) * sine


def backward_kernel(
    bounds, start_ref, cos_ref, sin_ref, q_ref, k_ref, v_ref, out_ref, grad_ref, lse_ref,
    dq_ref, dk_ref, dv_ref, bias_ref, dqt_ref, qt_ref, gt_ref, delta_ref,
):
    j = pl.program_id(1)
    blocks = q_ref.shape[0] // BLOCK

    @pl.when(j == 0)
    def _():
        bias_ref[...] = jnp.zeros_like(bias_ref)
        dqt_ref[...] = jnp.zeros_like(dqt_ref)

        @pl.loop(0, blocks)
        def _(i):
            at = pl.ds(pl.multiple_of(i * BLOCK, BLOCK), BLOCK)
            grad = grad_ref[at, :]
            qt_ref[:, at] = q_ref[at, :].T
            gt_ref[:, at] = grad.T
            both = (grad.astype(jnp.float32) * out_ref[at, :].astype(jnp.float32)).T
            delta_ref[:, at] = jnp.concatenate(
                [
                    jnp.sum(both[head * HD : (head + 1) * HD], axis=0, keepdims=True)
                    for head in range(2)
                ],
                axis=0,
            )

    key, value = k_ref[...], v_ref[...]
    key_t = key.T
    width = key.shape[1]

    def step(masked):
        def body(i, carry):
            at = pl.ds(pl.multiple_of(i * BLOCK, BLOCK), BLOCK)
            key_grad, value_grad = carry
            query, grad = q_ref[at, :], grad_ref[at, :]
            query_t, grad_t = qt_ref[:, at], gt_ref[:, at]
            if masked:
                allowed = allowed_tile(start_ref[:, at], j, i)
            for head in range(2):
                scores = jnp.dot(key, head_rows(query_t, head), preferred_element_type=jnp.float32)
                probs = jnp.exp2(
                    scores * (HD**-0.5 * LOG2E) - lse_ref[0, head : head + 1, at]
                )
                if masked:
                    probs = jnp.where(allowed, probs, 0.0)
                back = jnp.dot(value, head_rows(grad_t, head), preferred_element_type=jnp.float32)
                score_grad = (probs * (back - delta_ref[head : head + 1, at])).astype(jnp.bfloat16)
                value_grad = value_grad + jnp.dot(
                    probs.astype(jnp.bfloat16), head_lanes(grad, head), preferred_element_type=jnp.float32
                )
                key_grad = key_grad + jnp.dot(
                    score_grad, head_lanes(query, head), preferred_element_type=jnp.float32
                )
                dqt_ref[head * HD : (head + 1) * HD, at] += jnp.dot(
                    key_t[head * HD : (head + 1) * HD], score_grad, preferred_element_type=jnp.float32
                )
            return key_grad, value_grad

        return body

    zero = jnp.zeros((BLOCK, width), jnp.float32)
    whole, last = bounds[2, j], bounds[3, j]
    carry = step(True)(j, (zero, zero))
    carry = lax.fori_loop(j + 1, whole, step(False), carry)
    key_grad, value_grad = lax.fori_loop(whole, last, step(True), carry)
    here = pl.ds(pl.multiple_of(j * BLOCK, BLOCK), BLOCK)
    key_grad = turn(key_grad * HD**-0.5, cos_ref[here, :], sin_ref[here, :], -1.0)
    dk_ref[...] = key_grad.astype(jnp.bfloat16)
    dv_ref[...] = value_grad.astype(jnp.bfloat16)
    bias_ref[1:2, :] += jnp.sum(key_grad, axis=0, keepdims=True)
    bias_ref[2:3, :] += jnp.sum(value_grad, axis=0, keepdims=True)

    @pl.when(j == blocks - 1)
    def _():
        @pl.loop(0, blocks)
        def _(i):
            at = pl.ds(pl.multiple_of(i * BLOCK, BLOCK), BLOCK)
            query_grad = turn(dqt_ref[:, at].T * HD**-0.5, cos_ref[at, :], sin_ref[at, :], -1.0)
            dq_ref[at, :] = query_grad.astype(jnp.bfloat16)
            bias_ref[0:1, :] += jnp.sum(query_grad, axis=0, keepdims=True)


def attention_backward(bounds, start, cosine, sine, query, key, value, attended, grad, lse):
    length, cols = query.shape
    width = 2 * HD
    pairs, blocks = cols // width, length // BLOCK
    whole = pl.BlockSpec((length, width), lambda p, j, b: (0, p))
    block = pl.BlockSpec((BLOCK, width), lambda p, j, b: (j, p))
    table = pl.BlockSpec((length, width), lambda p, j, b: (0, 0))
    shape = jax.ShapeDtypeStruct((length, cols), jnp.bfloat16)
    return pl.pallas_call(
        backward_kernel,
        out_shape=(shape, shape, shape, jax.ShapeDtypeStruct((3, cols), jnp.float32)),
        grid_spec=pltpu.PrefetchScalarGridSpec(
            num_scalar_prefetch=1,
            grid=(pairs, blocks),
            in_specs=[
                pl.BlockSpec((1, length), lambda p, j, b: (0, 0)),
                table,
                table,
                whole,
                block,
                block,
                whole,
                whole,
                pl.BlockSpec((1, 2, length), lambda p, j, b: (p, 0, 0)),
            ],
            out_specs=(whole, block, block, pl.BlockSpec((3, width), lambda p, j, b: (0, p))),
            scratch_shapes=[
                pltpu.VMEM((width, length), jnp.float32),
                pltpu.VMEM((width, length), jnp.bfloat16),
                pltpu.VMEM((width, length), jnp.bfloat16),
                pltpu.VMEM((2, length), jnp.float32),
            ],
        ),
        compiler_params=pltpu.CompilerParams(dimension_semantics=("arbitrary", "arbitrary")),
        cost_estimate=pl.CostEstimate(
            flops=40 * 10**9, bytes_accessed=8 * 2 * length * cols, transcendentals=0
        ),
        name="attention_backward",
    )(bounds, start.reshape(1, length), cosine, sine, query, key, value, attended, grad, lse)


def project_kernel(hidden_ref, weight_ref, bias_ref, cos_ref, sin_ref, q_ref, k_ref, v_ref):
    hidden = hidden_ref[...]
    width = 2 * HD
    for part, out in enumerate((q_ref, k_ref, v_ref)):
        made = jnp.dot(hidden, weight_ref[part], preferred_element_type=jnp.float32)
        made = made + bias_ref[part : part + 1, :]
        for pair in range(made.shape[1] // width):
            lanes = slice(pair * width, (pair + 1) * width)
            piece = made[:, lanes]
            if part < 2:
                piece = turn(piece, cos_ref[...], sin_ref[...], 1.0)
            out[:, lanes] = piece.astype(jnp.bfloat16)


def project(hidden, weight, bias, cosine, sine):
    rows, depth = hidden.shape
    cols = weight.shape[2]
    width = 2 * HD
    made = jax.ShapeDtypeStruct((rows, cols), jnp.bfloat16)
    table = pl.BlockSpec((BLOCK, width), lambda i: (i, 0))
    out = pl.BlockSpec((BLOCK, cols), lambda i: (i, 0))
    return pl.pallas_call(
        project_kernel,
        out_shape=(made, made, made),
        grid=(rows // BLOCK,),
        in_specs=[
            pl.BlockSpec((BLOCK, depth), lambda i: (i, 0)),
            pl.BlockSpec((3, depth, cols), lambda i: (0, 0, 0)),
            pl.BlockSpec((3, cols), lambda i: (0, 0)),
            table,
            table,
        ],
        out_specs=(out, out, out),
        compiler_params=pltpu.CompilerParams(dimension_semantics=("arbitrary",)),
        cost_estimate=pl.CostEstimate(
            flops=2 * rows * depth * 3 * cols,
            bytes_accessed=2 * (rows * depth + 3 * depth * cols + 3 * rows * cols),
            transcendentals=0,
        ),
        name="project",
    )(hidden, weight, bias, cosine, sine)


def rotary_tables(segments, start):
    length = segments.shape[0]
    place = (jnp.arange(length, dtype=jnp.int32) - start).astype(jnp.float32)
    freq = 10000.0 ** (-(2.0 * jnp.arange(ROT // 2, dtype=jnp.float32)) / ROT)
    lane = jnp.arange(2 * HD, dtype=jnp.int32) % HD
    angle = place[:, None] * jnp.tile(freq, 2 * HD // (ROT // 2))[None, :]
    turned = (lane < ROT)[None, :]
    return jnp.where(turned, jnp.cos(angle), 1.0), jnp.where(turned, jnp.sin(angle), 0.0)


def local(
    sizes,
    block_in,
    ln_gain,
    ln_bias,
    qkv_weight,
    qkv_bias,
    out_weight,
    out_bias,
    up_weight,
    up_bias,
    down_weight,
    down_bias,
    segments,
    cotangent,
):
    dp, tensor = sizes
    depth = block_in.shape[1]
    units = up_weight.shape[1]
    cols = qkv_weight.shape[2]
    contract_rows = (((0,), (0,)), ((), ()))
    contract_cols = (((1,), (1,)), ((), ()))
    normed, inv_scale = normalize(block_in)
    hidden_own = (normed * ln_gain + ln_bias).astype(jnp.bfloat16)
    hidden = lax.all_gather(hidden_own, "tensor", axis=0, tiled=True)
    grad_out = lax.all_gather(cotangent, "tensor", axis=0, tiled=True)
    start, bounds = attention_bounds(segments)
    cosine, sine = rotary_tables(segments, start)
    query, key, value = project(hidden, qkv_weight, qkv_bias, cosine, sine)
    attended, log_sums = attention_forward(bounds, start, query, key, value)
    act_pre = jnp.dot(hidden, up_weight, preferred_element_type=jnp.float32) + up_bias
    act_value, act_slope = gelu_pair(act_pre)
    act = act_value.astype(jnp.bfloat16)
    slope = act_slope.astype(jnp.bfloat16)
    branch = lax.psum_scatter(
        (
            jnp.dot(attended, out_weight, preferred_element_type=jnp.float32)
            + jnp.dot(act, down_weight, preferred_element_type=jnp.float32)
        ).astype(jnp.bfloat16),
        "tensor",
        scatter_dimension=0,
        tiled=True,
    ).astype(jnp.float32)
    block_out = (block_in.astype(jnp.float32) + branch + out_bias + down_bias).astype(jnp.bfloat16)
    bias_sum = jnp.sum(grad_out.astype(jnp.float32), axis=0)
    down_grad = lax.dot_general(
        act, grad_out, contract_rows, preferred_element_type=jnp.float32
    ).astype(jnp.bfloat16)
    act_grad = lax.dot_general(
        grad_out, down_weight, contract_cols, preferred_element_type=jnp.float32
    ) * slope.astype(jnp.float32)
    up_bias_local = jnp.sum(act_grad, axis=0)
    act_grad_b = act_grad.astype(jnp.bfloat16)
    up_grad = lax.dot_general(
        hidden, act_grad_b, contract_rows, preferred_element_type=jnp.float32
    ).astype(jnp.bfloat16)
    out_grad = lax.dot_general(
        attended, grad_out, contract_rows, preferred_element_type=jnp.float32
    ).astype(jnp.bfloat16)
    attended_grad = lax.dot_general(
        grad_out, out_weight, contract_cols, preferred_element_type=jnp.float32
    ).astype(jnp.bfloat16)
    query_grad, key_grad, value_grad, qkv_bias_local = attention_backward(
        bounds, start, cosine, sine, query, key, value, attended, attended_grad, log_sums
    )
    parts = (query_grad, key_grad, value_grad)
    term = lax.dot_general(
        act_grad_b, up_weight, contract_cols, preferred_element_type=jnp.float32
    )
    for index, part in enumerate(parts):
        term = term + lax.dot_general(
            part, qkv_weight[index], contract_cols, preferred_element_type=jnp.float32
        )
    hidden_grad = lax.psum_scatter(
        term.astype(jnp.bfloat16), "tensor", scatter_dimension=0, tiled=True
    ).astype(jnp.float32)
    qkv_grads = [
        lax.dot_general(hidden, part, contract_rows, preferred_element_type=jnp.float32).astype(
            jnp.bfloat16
        )
        for part in parts
    ]
    down_share = lax.psum_scatter(
        down_grad, "dp", scatter_dimension=1, tiled=True
    ).astype(jnp.float32)
    up_share = lax.psum_scatter(up_grad, "dp", scatter_dimension=0, tiled=True).astype(jnp.float32)
    out_share = lax.psum_scatter(
        out_grad, "dp", scatter_dimension=1, tiled=True
    ).astype(jnp.float32)
    qkv_share = lax.psum_scatter(
        jnp.stack(qkv_grads), "dp", scatter_dimension=1, tiled=True
    ).astype(jnp.float32)
    early = small_sum(lanes_of(qkv_bias_local, up_bias_local, bias_sum), (("dp", dp),), 1)
    qkv_rows, up_rows = 3 * cols // 128, units // 128
    qkv_bias_grad = early[:qkv_rows].reshape(3, cols)
    up_bias_grad = early[qkv_rows : qkv_rows + up_rows].reshape(units)
    bias_total = early[qkv_rows + up_rows :].reshape(depth)
    gain_local = jnp.sum(hidden_grad * normed, axis=0)
    shift_local = jnp.sum(hidden_grad, axis=0)
    late = small_sum(lanes_of(gain_local, shift_local), (("tensor", tensor), ("dp", dp)), 2)
    gain_grad, shift_grad = late.reshape(2, depth)
    scaled = hidden_grad * ln_gain
    inner = (
        scaled
        - jnp.mean(scaled, axis=-1, keepdims=True)
        - normed * jnp.mean(scaled * normed, axis=-1, keepdims=True)
    )
    input_grad = (cotangent.astype(jnp.float32) + inv_scale * inner).astype(jnp.bfloat16)
    return (
        block_out,
        input_grad,
        gain_grad,
        shift_grad,
        qkv_share,
        qkv_bias_grad,
        out_share,
        bias_total,
        up_share,
        up_bias_grad,
        down_share,
        bias_total,
    )


def solution(mesh):
    return jax.shard_map(
        functools.partial(local, (mesh.shape["dp"], mesh.shape["tensor"])),
        mesh=mesh,
        in_specs=(
            P(("dp", "tensor"), None),
            P(),
            P(),
            P(None, None, "tensor"),
            P(None, "tensor"),
            P("tensor", None),
            P(),
            P(None, "tensor"),
            P("tensor"),
            P("tensor", None),
            P(),
            P("dp"),
            P(("dp", "tensor"), None),
        ),
        out_specs=(
            P(("dp", "tensor"), None),
            P(("dp", "tensor"), None),
            P(),
            P(),
            P(None, "dp", "tensor"),
            P(None, "tensor"),
            P("tensor", "dp"),
            P(),
            P("dp", "tensor"),
            P("tensor"),
            P("tensor", "dp"),
            P(),
        ),
        check_vma=False,
    )
```

```python
import functools

import jax
import jax.numpy as jnp
from jax import lax
from jax.experimental import pallas as pl
from jax.experimental.pallas import tpu as pltpu
from jax.sharding import PartitionSpec as P


HD = 64
ROT = 32

EPSILON = 1e-05
NEGATIVE = -1e30
ROOT_TWO_PI = 0.7978845608028654
MESH = pl.DeviceIdType.MESH


def normalize(rows):
    wide = rows.astype(jnp.float32)
    centre = wide - jnp.mean(wide, axis=-1, keepdims=True)
    inv_scale = lax.rsqrt(jnp.mean(centre * centre, axis=-1, keepdims=True) + EPSILON)
    return (centre * inv_scale, inv_scale)


def gelu_pair(pre):
    inner = ROOT_TWO_PI * (pre + 0.044715 * pre * pre * pre)
    tangent = jnp.tanh(inner)
    value = 0.5 * pre * (1.0 + tangent)
    slope = 0.5 * (1.0 + tangent) + 0.5 * pre * (1.0 - tangent * tangent) * ROOT_TWO_PI * (
        1.0 + 3.0 * 0.044715 * pre * pre
    )
    return (value, slope)


def sum_kernel(axes, x_ref, out_ref, *scratch):
    barrier = pltpu.get_barrier_semaphore()
    peers = 0
    for name, size in axes:
        me = lax.axis_index(name)
        for step in range(1, size):
            pl.semaphore_signal(
                barrier, inc=1, device_id={name: lax.rem(me + step, size)}, device_id_type=MESH
            )
            peers += 1
    pl.semaphore_wait(barrier, peers)
    held = x_ref
    for number, (name, size) in enumerate(axes):
        slots, total, send, receive = scratch[4 * number : 4 * number + 4]
        me = lax.axis_index(name)
        copies = []
        for step in range(1, size):
            copy = pltpu.make_async_remote_copy(
                src_ref=held,
                dst_ref=slots.at[step - 1],
                send_sem=send.at[step - 1],
                recv_sem=receive.at[step - 1],
                device_id={name: lax.rem(me + step, size)},
                device_id_type=MESH,
            )
            copy.start()
            copies.append(copy)
        for copy in copies:
            copy.wait()
        made = jnp.zeros(x_ref.shape, jnp.float32)
        for device in range(size):
            piece = jnp.where(me == device, held[...], 0.0)
            for step in range(1, size):
                piece = piece + jnp.where(
                    lax.rem(me + size - step, size) == device, slots[step - 1], 0.0
                )
            made = made + piece
        total[...] = made
        held = total
    out_ref[...] = held[...]


def small_sum(values, axes, collective_id):
    scratch = []
    for _, size in axes:
        scratch += [
            pltpu.VMEM((size - 1, *values.shape), jnp.float32),
            pltpu.VMEM(values.shape, jnp.float32),
            pltpu.SemaphoreType.DMA((size - 1,)),
            pltpu.SemaphoreType.DMA((size - 1,)),
        ]
    return pl.pallas_call(
        functools.partial(sum_kernel, axes),
        out_shape=jax.ShapeDtypeStruct(values.shape, jnp.float32),
        in_specs=[pl.BlockSpec(memory_space=pltpu.VMEM)],
        out_specs=pl.BlockSpec(memory_space=pltpu.VMEM),
        scratch_shapes=scratch,
        compiler_params=pltpu.CompilerParams(collective_id=collective_id, has_side_effects=True),
        name="small_sum",
    )(values)


def lanes_of(*parts):
    return jnp.concatenate([part.reshape(-1, 128) for part in parts], axis=0)


LOG2E = 1.4426950408889634
BLOCK = 256


def attention_tasks(segments, place, slots):
    length = segments.shape[0]
    begins = jnp.sum(
        (segments[None, :] < jnp.arange(1, 4, dtype=jnp.int32)[:, None]).astype(jnp.int32), axis=1
    )
    start = jnp.zeros_like(segments)
    for number in range(1, 4):
        start = jnp.where(segments == number, begins[number - 1], start)
    blocks = length // BLOCK
    first = start.reshape(blocks, BLOCK)[:, 0] // BLOCK
    entry = jnp.arange(blocks * blocks, dtype=jnp.int32)
    query, key = entry // blocks, lax.rem(entry, blocks)
    lowest = jnp.repeat(first, blocks)
    valid = (key <= query) & (key >= lowest)
    ahead = jnp.sum((valid[None, :] & (entry[None, :] < entry[:, None])).astype(jnp.int32), axis=1)
    count = jnp.sum(valid.astype(jnp.int32))
    room = blocks * (blocks + 1) // 2 + 4
    task = jnp.arange(room, dtype=jnp.int32)
    chosen = valid[None, :] & (ahead[None, :] == task[:, None])
    pick = lambda values: jnp.sum(jnp.where(chosen, values[None, :], 0), axis=1)
    per = blocks // slots
    lies = lambda block: lax.rem(place - block // per + slots, slots) * per + lax.rem(block, per)
    rows = [pick(query), jnp.where(task < count, pick(key), 1)]
    rows += [lies(rows[0]), lies(rows[1]), lies(lax.rem(task, blocks)), jnp.full_like(task, count)]
    return start, jnp.stack(rows)


def natural(block):
    return pl.ds(pl.multiple_of(block * BLOCK, BLOCK), BLOCK)


def head_rows(values, head):
    row = lax.broadcasted_iota(jnp.int32, values.shape, 0)
    return jnp.where(row // HD == head, values, jnp.zeros_like(values))


def head_lanes(values, head):
    lane = lax.broadcasted_iota(jnp.int32, values.shape, 1)
    return jnp.where(lane // HD == head, values, jnp.zeros_like(values))


def allowed_tile(start_row, key_block, query_block):
    key_index = lax.broadcasted_iota(jnp.int32, (BLOCK, BLOCK), 0)
    query_index = lax.broadcasted_iota(jnp.int32, (1, BLOCK), 1)
    last = (query_block - key_block) * BLOCK + query_index
    return (key_index <= last) & (key_index >= start_row - key_block * BLOCK)


def pipelined(tasks, stage_a, stage_b, stage_c):
    pairs = (tasks[5, 0] + 1) // 2
    stage_a(0, 0)

    @pl.loop(0, pairs)
    def _(pair):
        for half in range(2):
            task = 2 * pair + half
            stage_a(task + 1, 1 - half)
            stage_c(jnp.maximum(task - 1, 0), 1 - half)
            stage_b(task, half)

    stage_c(2 * pairs - 1, 1)


def forward_kernel(
    tasks, start_ref, q_ref, k_ref, v_ref, out_ref, lse_ref,
    qt_ref, vt_ref, acc_ref, peak_ref, total_ref, *slots,
):
    blocks = k_ref.shape[0] // BLOCK
    scores_ref, probs_ref, shrink_ref = slots[0:2], slots[2:4], slots[4:6]
    scale = HD**-0.5 * LOG2E
    peak_ref[...] = jnp.full_like(peak_ref, NEGATIVE)
    total_ref[...] = jnp.zeros_like(total_ref)
    acc_ref[...] = jnp.zeros_like(acc_ref)
    probs_ref[1][...] = jnp.zeros_like(probs_ref[1])
    shrink_ref[1][...] = jnp.ones_like(shrink_ref[1])

    @pl.loop(0, blocks)
    def _(b):
        at, held = natural(b), natural(tasks[4, b])
        vt_ref[:, at] = v_ref[held, :].T
        query = q_ref[held, :].T
        for head in range(2):
            qt_ref[head, :, at] = head_rows(query, head)

    def stage_a(task, slot):
        key = k_ref[natural(tasks[3, task]), :]
        for head in range(2):
            scores_ref[slot][head] = jnp.dot(
                key, qt_ref[head, :, natural(tasks[0, task])], preferred_element_type=jnp.float32
            )

    def stage_b(task, slot):
        i, j = tasks[0, task], tasks[1, task]
        at = natural(i)
        allowed = allowed_tile(start_ref[:, at], j, i)
        for head in range(2):
            row = slice(head, head + 1)
            scores = jnp.where(allowed, scores_ref[slot][head], NEGATIVE)
            peak = peak_ref[row, at]
            top = jnp.maximum(peak, jnp.max(scores, axis=0, keepdims=True))
            probs = jnp.exp2(scores * scale - top * scale)
            shrink = jnp.exp2((peak - top) * scale)
            peak_ref[row, at] = top
            total_ref[row, at] = total_ref[row, at] * shrink + jnp.sum(probs, axis=0, keepdims=True)
            shrink_ref[slot][row, :] = shrink
            probs_ref[slot][head] = probs.astype(jnp.bfloat16)

    def stage_c(task, slot):
        at, keys = natural(tasks[0, task]), natural(tasks[1, task])
        for head in range(2):
            rows = slice(head * HD, (head + 1) * HD)
            acc_ref[rows, at] = acc_ref[rows, at] * shrink_ref[slot][head : head + 1, :] + jnp.dot(
                vt_ref[rows, keys], probs_ref[slot][head], preferred_element_type=jnp.float32
            )

    pipelined(tasks, stage_a, stage_b, stage_c)

    @pl.loop(0, blocks)
    def _(b):
        at = natural(b)
        rows = [
            acc_ref[head * HD : (head + 1) * HD, at] / total_ref[head : head + 1, at]
            for head in range(2)
        ]
        out_ref[natural(tasks[4, b]), :] = jnp.concatenate(rows, axis=0).T.astype(jnp.bfloat16)
        lse_ref[0, :, at] = peak_ref[:, at] * scale + jnp.log2(total_ref[:, at])


def attention_forward(tasks, start, query, key, value):
    length, cols = query.shape
    width = 2 * HD
    pairs = cols // width
    whole = pl.BlockSpec((length, width), lambda p, b: (0, p))
    square = (2, BLOCK, BLOCK)
    return pl.pallas_call(
        forward_kernel,
        out_shape=(
            jax.ShapeDtypeStruct((length, cols), jnp.bfloat16),
            jax.ShapeDtypeStruct((pairs, 2, length), jnp.float32),
        ),
        grid_spec=pltpu.PrefetchScalarGridSpec(
            num_scalar_prefetch=1,
            grid=(pairs,),
            in_specs=[pl.BlockSpec((1, length), lambda p, b: (0, 0)), whole, whole, whole],
            out_specs=(whole, pl.BlockSpec((1, 2, length), lambda p, b: (p, 0, 0))),
            scratch_shapes=[
                pltpu.VMEM((2, width, length), jnp.bfloat16),
                pltpu.VMEM((width, length), jnp.bfloat16),
                pltpu.VMEM((width, length), jnp.float32),
                pltpu.VMEM((2, length), jnp.float32),
                pltpu.VMEM((2, length), jnp.float32),
            ]
            + [pltpu.VMEM(square, jnp.float32)] * 2
            + [pltpu.VMEM(square, jnp.bfloat16)] * 2
            + [pltpu.VMEM((2, BLOCK), jnp.float32)] * 2,
        ),
        compiler_params=pltpu.CompilerParams(dimension_semantics=("arbitrary",)),
        cost_estimate=pl.CostEstimate(
            flops=16 * 10**9, bytes_accessed=4 * 2 * length * cols, transcendentals=0
        ),
        name="attention_forward",
    )(tasks, start.reshape(1, length), query, key, value)


def turn(values, cosine, sine, sign):
    lane = lax.broadcasted_iota(jnp.int32, values.shape, 1)
    half = ROT // 2
    right = pltpu.roll(values, half, 1)
    left = pltpu.roll(values, values.shape[1] - half, 1)
    mixed = jnp.where(lane % HD < half, -left, right)
    return values * cosine + (sign * mixed) * sine


def backward_kernel(
    carried, tasks, start_ref, cos_ref, sin_ref, q_ref, k_ref, v_ref, out_ref, grad_ref, lse_ref, *refs
):
    dq_ref, dk_ref, dv_ref, bias_ref = refs[carried : carried + 4]
    qt_ref, gt_ref, kt_ref, dqt_ref, dka_ref, dva_ref, delta_ref, *slots = refs[carried + 4 :]
    blocks = q_ref.shape[0] // BLOCK
    scores_ref, back_ref, probs_ref, sgrad_ref = slots[0:2], slots[2:4], slots[4:6], slots[6:8]
    scale = HD**-0.5 * LOG2E
    dqt_ref[...] = jnp.zeros_like(dqt_ref)
    dka_ref[...] = jnp.zeros_like(dka_ref)
    dva_ref[...] = jnp.zeros_like(dva_ref)
    bias_ref[...] = jnp.zeros_like(bias_ref)
    probs_ref[1][...] = jnp.zeros_like(probs_ref[1])
    sgrad_ref[1][...] = jnp.zeros_like(sgrad_ref[1])

    @pl.loop(0, blocks)
    def _(b):
        at, held = natural(b), natural(tasks[4, b])
        grad = grad_ref[held, :]
        query_t, grad_t = q_ref[held, :].T, grad.T
        kt_ref[:, at] = k_ref[held, :].T
        both = (grad.astype(jnp.float32) * out_ref[held, :].astype(jnp.float32)).T
        for head in range(2):
            qt_ref[head, :, at] = head_rows(query_t, head)
            gt_ref[head, :, at] = head_rows(grad_t, head)
            delta_ref[head : head + 1, at] = jnp.sum(
                both[head * HD : (head + 1) * HD], axis=0, keepdims=True
            )

    def stage_a(task, slot):
        at, keys = natural(tasks[0, task]), natural(tasks[3, task])
        key, value = k_ref[keys, :], v_ref[keys, :]
        for head in range(2):
            scores_ref[slot][head] = jnp.dot(
                key, qt_ref[head, :, at], preferred_element_type=jnp.float32
            )
            back_ref[slot][head] = jnp.dot(
                value, gt_ref[head, :, at], preferred_element_type=jnp.float32
            )

    def stage_b(task, slot):
        i, j = tasks[0, task], tasks[1, task]
        at = natural(i)
        allowed = allowed_tile(start_ref[:, at], j, i)
        for head in range(2):
            probs = jnp.exp2(scores_ref[slot][head] * scale - lse_ref[0, head : head + 1, at])
            probs = jnp.where(allowed, probs, 0.0)
            probs_ref[slot][head] = probs.astype(jnp.bfloat16)
            sgrad_ref[slot][head] = (
                probs * (back_ref[slot][head] - delta_ref[head : head + 1, at])
            ).astype(jnp.bfloat16)

    def stage_c(task, slot):
        at, keys = natural(tasks[0, task]), natural(tasks[1, task])
        held = natural(tasks[2, task])
        query, grad = q_ref[held, :], grad_ref[held, :]
        for target, left, right in ((dva_ref, probs_ref, grad), (dka_ref, sgrad_ref, query)):
            target[keys, :] += sum(
                jnp.dot(
                    left[slot][head], head_lanes(right, head), preferred_element_type=jnp.float32
                )
                for head in range(2)
            )
        for head in range(2):
            rows = slice(head * HD, (head + 1) * HD)
            dqt_ref[rows, at] += jnp.dot(
                kt_ref[rows, keys], sgrad_ref[slot][head], preferred_element_type=jnp.float32
            )

    pipelined(tasks, stage_a, stage_b, stage_c)

    @pl.loop(0, blocks)
    def _(b):
        at, held = natural(b), natural(tasks[4, b])
        cosine, sine = cos_ref[at, :], sin_ref[at, :]
        grads = (
            turn(dqt_ref[:, at].T * HD**-0.5, cosine, sine, -1.0),
            turn(dka_ref[at, :] * HD**-0.5, cosine, sine, -1.0),
            dva_ref[at, :],
        )
        for part, (out, grad) in enumerate(zip((dq_ref, dk_ref, dv_ref), grads)):
            out[held, :] = grad.astype(jnp.bfloat16)
            bias_ref[part : part + 1, :] += jnp.sum(grad, axis=0, keepdims=True)


def attention_backward(
    part, tasks, start, cosine, sine, query, key, value, attended, grad, lse, before
):
    length, cols = query.shape
    width = 2 * HD
    first, pairs = part
    whole = pl.BlockSpec((length, width), lambda p, b: (0, first + p))
    table = pl.BlockSpec((length, width), lambda p, b: (0, 0))
    shape = jax.ShapeDtypeStruct((length, cols), jnp.bfloat16)
    square = (2, BLOCK, BLOCK)
    carried = len(before)
    return pl.pallas_call(
        functools.partial(backward_kernel, carried),
        out_shape=(shape, shape, shape, jax.ShapeDtypeStruct((3, cols), jnp.float32)),
        grid_spec=pltpu.PrefetchScalarGridSpec(
            num_scalar_prefetch=1,
            grid=(pairs,),
            in_specs=[
                pl.BlockSpec((1, length), lambda p, b: (0, 0)),
                table,
                table,
                whole,
                whole,
                whole,
                whole,
                whole,
                pl.BlockSpec((1, 2, length), lambda p, b: (first + p, 0, 0)),
            ]
            + [pl.BlockSpec(memory_space=pl.ANY)] * carried,
            out_specs=(whole, whole, whole, pl.BlockSpec((3, width), lambda p, b: (0, first + p))),
            scratch_shapes=[
                pltpu.VMEM((2, width, length), jnp.bfloat16),
                pltpu.VMEM((2, width, length), jnp.bfloat16),
                pltpu.VMEM((width, length), jnp.bfloat16),
                pltpu.VMEM((width, length), jnp.float32),
                pltpu.VMEM((length, width), jnp.float32),
                pltpu.VMEM((length, width), jnp.float32),
                pltpu.VMEM((2, length), jnp.float32),
            ]
            + [pltpu.VMEM(square, jnp.float32)] * 4
            + [pltpu.VMEM(square, jnp.bfloat16)] * 4,
        ),
        input_output_aliases={10 + i: i for i in range(carried)},
        compiler_params=pltpu.CompilerParams(dimension_semantics=("arbitrary",)),
        cost_estimate=pl.CostEstimate(
            flops=10**10 * pairs, bytes_accessed=8 * 2 * length * width * pairs, transcendentals=0
        ),
        name="attention_backward",
    )(tasks, start.reshape(1, length), cosine, sine, query, key, value, attended, grad, lse, *before)


def rotary_tables(segments, start):
    length = segments.shape[0]
    place = (jnp.arange(length, dtype=jnp.int32) - start).astype(jnp.float32)
    freq = 10000.0 ** (-(2.0 * jnp.arange(ROT // 2, dtype=jnp.float32)) / ROT)
    lane = jnp.arange(2 * HD, dtype=jnp.int32) % HD
    angle = place[:, None] * jnp.tile(freq, 2 * HD // (ROT // 2))[None, :]
    turned = (lane < ROT)[None, :]
    return jnp.where(turned, jnp.cos(angle), 1.0), jnp.where(turned, jnp.sin(angle), 0.0)


TILE = 1024


def dot_nt(left, right):
    return lax.dot_general(left, right, (((1,), (1,)), ((), ())), preferred_element_type=jnp.float32)


def chunk_kernel(
    hidden_ref, qkv_ref, bias_ref, cos_ref, sin_ref, up_ref, up_bias_ref, *refs
):
    q_ref, k_ref, v_ref, act_ref, slope_ref, all_ref = refs[-6:]
    step = pl.program_id(0)
    width = 2 * HD

    @pl.when(step == 0)
    def _():
        all_ref[...] = hidden_ref[...]
        for part, out in enumerate((q_ref, k_ref, v_ref)):
            made = jnp.dot(hidden_ref[...], qkv_ref[part], preferred_element_type=jnp.float32)
            made = made + bias_ref[part : part + 1, :]
            for pair in range(made.shape[1] // width):
                lanes = slice(pair * width, (pair + 1) * width)
                piece = made[:, lanes]
                if part < 2:
                    piece = turn(piece, cos_ref[...], sin_ref[...], 1.0)
                out[:, lanes] = piece.astype(jnp.bfloat16)

    @pl.when(step > 0)
    def _():
        made = jnp.dot(hidden_ref[...], up_ref[...], preferred_element_type=jnp.float32)
        value, slope = gelu_pair(made + up_bias_ref[...])
        act_ref[...] = value.astype(jnp.bfloat16)
        slope_ref[...] = slope.astype(jnp.bfloat16)


def chunk_forward(slot, slots, hidden, weight, bias, cosine, sine, up_weight, up_bias, before):
    rows, depth = hidden.shape
    cols, units = weight.shape[2], up_weight.shape[1]
    width = 2 * HD
    tile = min(TILE, units)
    tiles = units // tile
    length = slots * rows
    made = [jax.ShapeDtypeStruct((length, n), jnp.bfloat16) for n in (cols, cols, cols, units, units, depth)]
    table = pl.BlockSpec((rows, width), lambda s: (0, 0))
    unit = lambda s: jnp.maximum(s - 1, 0)
    out = pl.BlockSpec((rows, cols), lambda s: (slot, 0))
    wide = pl.BlockSpec((rows, tile), lambda s: (slot, unit(s)))
    extra = list(before) if before is not None else []
    return pl.pallas_call(
        chunk_kernel,
        out_shape=made,
        grid=(1 + tiles,),
        in_specs=[
            pl.BlockSpec((rows, depth), lambda s: (0, 0)),
            pl.BlockSpec((3, depth, cols), lambda s: (0, 0, 0)),
            pl.BlockSpec((3, cols), lambda s: (0, 0)),
            table,
            table,
            pl.BlockSpec((depth, tile), lambda s: (0, unit(s))),
            pl.BlockSpec((1, tile), lambda s: (0, unit(s))),
        ]
        + [pl.BlockSpec(memory_space=pl.ANY)] * len(extra),
        out_specs=[out, out, out, wide, wide, pl.BlockSpec((rows, depth), lambda s: (slot, 0))],
        input_output_aliases={7 + i: i for i in range(len(extra))},
        compiler_params=pltpu.CompilerParams(dimension_semantics=("arbitrary",)),
        cost_estimate=pl.CostEstimate(
            flops=2 * rows * depth * (3 * cols + units),
            bytes_accessed=2 * (2 * rows * depth + depth * (3 * cols + units) + rows * (3 * cols + 2 * units)),
            transcendentals=rows * units,
        ),
        name="chunk_forward",
    )(hidden, weight, bias, cosine, sine, up_weight, up_bias.reshape(1, units), *extra)


def parts_kernel(count, transposed, *refs):
    total = None
    out_ref = refs[2 * count]
    for left, right in zip(refs[:count], refs[count : 2 * count]):
        weight = right[0] if len(right.shape) == 3 else right[...]
        made = (dot_nt if transposed else functools.partial(jnp.dot, preferred_element_type=jnp.float32))(
            left[...], weight
        )
        total = made if total is None else total + made
    out_ref[...] = total.astype(jnp.bfloat16)


def parts_matmul(slots, rows, lefts, rights, transposed):
    count = len(lefts)
    columns = rights[-1][0].shape[-2 if transposed else -1]
    tile = min(TILE, columns)
    first, second = slots[0], slots[-1]
    pick = (lambda r: first + r * (second - first)) if len(slots) > 1 else (lambda r: first)
    in_specs = [pl.BlockSpec((rows, left.shape[1]), lambda r, n: (pick(r), 0)) for left in lefts]
    work = 0
    for right, part in rights:
        depth = right.shape[-1] if transposed else right.shape[-2]
        work += depth
        shape = (tile, depth) if transposed else (depth, tile)
        at = (lambda n: (n, 0)) if transposed else (lambda n: (0, n))
        if part is None:
            in_specs.append(pl.BlockSpec(shape, lambda r, n, at=at: at(n)))
        else:
            in_specs.append(pl.BlockSpec((1, *shape), lambda r, n, at=at, part=part: (part, *at(n))))
    height = len(slots) * rows
    return pl.pallas_call(
        functools.partial(parts_kernel, count, transposed),
        out_shape=jax.ShapeDtypeStruct((height, columns), jnp.bfloat16),
        grid=(len(slots), columns // tile),
        in_specs=in_specs,
        out_specs=pl.BlockSpec((rows, tile), lambda r, n: (r, n)),
        compiler_params=pltpu.CompilerParams(dimension_semantics=("arbitrary", "arbitrary")),
        cost_estimate=pl.CostEstimate(
            flops=2 * height * work * columns,
            bytes_accessed=2 * (height * work + work * columns + height * columns),
            transcendentals=0,
        ),
    )(*lefts, *(right for right, _ in rights))


def act_grad_kernel(grad_ref, down_ref, slope_ref, out_ref, sum_ref):
    made = dot_nt(grad_ref[...], down_ref[...]) * slope_ref[...].astype(jnp.float32)
    out_ref[...] = made.astype(jnp.bfloat16)

    @pl.when(pl.program_id(1) == 0)
    def _():
        sum_ref[...] = jnp.zeros_like(sum_ref)

    sum_ref[...] += jnp.sum(made, axis=0, keepdims=True)


def act_gradient(grad_out, down_weight, slope, rows):
    length, depth = grad_out.shape
    units = down_weight.shape[0]
    tile = min(TILE, units)
    rows = min(2 * rows, length)
    wide = pl.BlockSpec((rows, tile), lambda n, r: (r, n))
    return pl.pallas_call(
        act_grad_kernel,
        out_shape=(
            jax.ShapeDtypeStruct((length, units), jnp.bfloat16),
            jax.ShapeDtypeStruct((1, units), jnp.float32),
        ),
        grid=(units // tile, length // rows),
        in_specs=[
            pl.BlockSpec((rows, depth), lambda n, r: (r, 0)),
            pl.BlockSpec((tile, depth), lambda n, r: (n, 0)),
            wide,
        ],
        out_specs=(wide, pl.BlockSpec((1, tile), lambda n, r: (0, n))),
        compiler_params=pltpu.CompilerParams(dimension_semantics=("arbitrary", "arbitrary")),
        cost_estimate=pl.CostEstimate(
            flops=2 * length * depth * units,
            bytes_accessed=2 * (length * depth + depth * units + 2 * length * units),
            transcendentals=0,
        ),
        name="act_gradient",
    )(grad_out, down_weight, slope)


def line(size, right, step):
    return [(i, i + 1 if right else i - 1) for i in step if 0 <= (i + 1 if right else i - 1) < size]


def ring_gather(own, size):
    pairs = [(i, (i + 1) % size) for i in range(size)]
    slots = [own]
    for _ in range(1, size):
        slots.append(lax.ppermute(slots[-1], "tensor", pairs))
    return slots


def line_gather(own, size):
    from_left, from_right = [own], [own]
    for step in range(1, size):
        from_left.append(
            lax.ppermute(from_left[-1], "tensor", line(size, True, range(step - 1, size)))
        )
        from_right.append(
            lax.ppermute(from_right[-1], "tensor", line(size, False, range(size - step + 1)))
        )
    return [own] + [from_left[step] + from_right[size - step] for step in range(1, size)]


def line_scatter(slots, size):
    right = left = None
    for step in range(1, size):
        go_right, go_left = slots[step], slots[size - step]
        if step > 1:
            go_right, go_left = go_right + right, go_left + left
        right = lax.ppermute(go_right, "tensor", line(size, True, range(step)))
        left = lax.ppermute(go_left, "tensor", line(size, False, range(size - step, size)))
    return right, left


def slot_order(size):
    order = []
    for step in range(1, size):
        for slot in (step, size - step):
            if slot not in order:
                order.append(slot)
    order.append(0)
    return [tuple(order[i : i + 2]) for i in range(0, size, 2)]


def by_slot(groups, rows, make):
    slots = {}
    for group in groups:
        made = make(group)
        for place, slot in enumerate(group):
            slots[slot] = made[place * rows : (place + 1) * rows]
    return [slots[slot] for slot in range(len(slots))]


def layer(
    sizes,
    block_in,
    ln_gain,
    ln_bias,
    qkv_weight,
    qkv_bias,
    out_weight,
    out_bias,
    up_weight,
    up_bias,
    down_weight,
    down_bias,
    segments,
    cotangent,
):
    dp, tensor = sizes
    depth = block_in.shape[1]
    units = up_weight.shape[1]
    cols = qkv_weight.shape[2]
    contract_rows = (((0,), (0,)), ((), ()))
    contract_cols = (((1,), (1,)), ((), ()))
    rows = block_in.shape[0]
    place = lax.axis_index("tensor")
    normed, inv_scale = normalize(block_in)
    hidden_own = (normed * ln_gain + ln_bias).astype(jnp.bfloat16)
    chunks = ring_gather(hidden_own, tensor)
    start, tasks = attention_tasks(segments, place, tensor)
    cosine, sine = rotary_tables(segments, start)
    made = None
    for slot, chunk in enumerate(chunks):
        offset = lax.rem(place - slot + tensor, tensor) * rows
        turned = [lax.dynamic_slice_in_dim(table, offset, rows, 0) for table in (cosine, sine)]
        made = chunk_forward(
            slot, tensor, chunk, qkv_weight, qkv_bias, *turned, up_weight, up_bias, made
        )
    query, key, value, act, slope, hidden = made
    grad_own, _ = lax.optimization_barrier((cotangent, chunks[-1]))
    grad_out = jnp.concatenate(line_gather(grad_own, tensor), axis=0)
    attended, log_sums = attention_forward(tasks, start, query, key, value)
    groups = slot_order(tensor)
    branch = by_slot(
        groups,
        rows,
        lambda group: parts_matmul(group, rows, (attended, act), ((out_weight, None), (down_weight, None)), False),
    )
    right, left = line_scatter(branch, tensor)
    wide = [part.astype(jnp.float32) for part in (branch[0], right, left)]
    block_out = (
        block_in.astype(jnp.float32) + (wide[0] + wide[1] + wide[2]) + out_bias + down_bias
    ).astype(jnp.bfloat16)
    bias_sum = jnp.sum(cotangent.astype(jnp.float32), axis=0)
    act_grad, up_bias_local = act_gradient(grad_out, down_weight, slope, rows)
    down_grad = lax.dot_general(act, grad_out, contract_rows, preferred_element_type=jnp.float32).astype(jnp.bfloat16)
    attended_grad = lax.dot_general(
        grad_out, out_weight, contract_cols, preferred_element_type=jnp.float32
    ).astype(jnp.bfloat16)
    back = []
    pairs = cols // (2 * HD)
    for half in range(2):
        back = attention_backward(
            (half * (pairs // 2), pairs // 2),
            tasks, start, cosine, sine, query, key, value, attended, attended_grad, log_sums, back,
        )
    *parts, qkv_bias_local = back
    hidden_parts = by_slot(
        groups,
        rows,
        lambda group: parts_matmul(
            group,
            rows,
            (*parts, act_grad),
            ((qkv_weight, 0), (qkv_weight, 1), (qkv_weight, 2), (up_weight, None)),
            True,
        ),
    )
    right, left = line_scatter(hidden_parts, tensor)
    wide = [part.astype(jnp.float32) for part in (hidden_parts[0], right, left)]
    hidden_grad = wide[0] + wide[1] + wide[2]
    up_grad = lax.dot_general(hidden, act_grad, contract_rows, preferred_element_type=jnp.float32).astype(jnp.bfloat16)
    cols_grad = jnp.stack(
        [
            lax.dot_general(left, right, contract_rows, preferred_element_type=jnp.float32).astype(
                jnp.bfloat16
            )
            for left, right in [(hidden, part) for part in parts] + [(grad_out, attended)]
        ]
    )
    down_share = lax.psum_scatter(
        down_grad, "dp", scatter_dimension=1, tiled=True
    ).astype(jnp.float32)
    up_share = lax.psum_scatter(up_grad, "dp", scatter_dimension=0, tiled=True).astype(jnp.float32)
    cols_share = lax.psum_scatter(
        cols_grad, "dp", scatter_dimension=1, tiled=True
    ).astype(jnp.float32)
    qkv_share, out_share = cols_share[:3], cols_share[3].T
    early = small_sum(lanes_of(qkv_bias_local, up_bias_local), (("dp", dp),), 1)
    qkv_rows = 3 * cols // 128
    qkv_bias_grad = early[:qkv_rows].reshape(3, cols)
    up_bias_grad = early[qkv_rows:].reshape(units)
    gain_local = jnp.sum(hidden_grad * normed, axis=0)
    shift_local = jnp.sum(hidden_grad, axis=0)
    late = small_sum(
        lanes_of(gain_local, shift_local, bias_sum), (("tensor", tensor), ("dp", dp)), 2
    )
    gain_grad, shift_grad, bias_total = late.reshape(3, depth)
    scaled = hidden_grad * ln_gain
    inner = (
        scaled
        - jnp.mean(scaled, axis=-1, keepdims=True)
        - normed * jnp.mean(scaled * normed, axis=-1, keepdims=True)
    )
    input_grad = (cotangent.astype(jnp.float32) + inv_scale * inner).astype(jnp.bfloat16)
    return (
        block_out,
        input_grad,
        gain_grad,
        shift_grad,
        qkv_share,
        qkv_bias_grad,
        out_share,
        bias_total,
        up_share,
        up_bias_grad,
        down_share,
        bias_total,
    )


def local(sizes, *arrays):
    return layer(sizes, *arrays)


def solution(mesh):
    return jax.shard_map(
        functools.partial(local, (mesh.shape["dp"], mesh.shape["tensor"])),
        mesh=mesh,
        in_specs=(
            P(("dp", "tensor"), None),
            P(),
            P(),
            P(None, None, "tensor"),
            P(None, "tensor"),
            P("tensor", None),
            P(),
            P(None, "tensor"),
            P("tensor"),
            P("tensor", None),
            P(),
            P("dp"),
            P(("dp", "tensor"), None),
        ),
        out_specs=(
            P(("dp", "tensor"), None),
            P(("dp", "tensor"), None),
            P(),
            P(),
            P(None, "dp", "tensor"),
            P(None, "tensor"),
            P("tensor", "dp"),
            P(),
            P("dp", "tensor"),
            P("tensor"),
            P("tensor", "dp"),
            P(),
        ),
        check_vma=False,
    )
```

```python
import functools

import jax
import jax.numpy as jnp
from jax import lax
from jax.experimental import pallas as pl
from jax.experimental.pallas import tpu as pltpu
from jax.sharding import PartitionSpec as P


HD = 64
ROT = 32

EPSILON = 1e-05
NEGATIVE = -1e30
ROOT_TWO_PI = 0.7978845608028654
MESH = pl.DeviceIdType.MESH


def normalize(rows):
    wide = rows.astype(jnp.float32)
    centre = wide - jnp.mean(wide, axis=-1, keepdims=True)
    inv_scale = lax.rsqrt(jnp.mean(centre * centre, axis=-1, keepdims=True) + EPSILON)
    return (centre * inv_scale, inv_scale)


def gelu_pair(pre):
    inner = ROOT_TWO_PI * (pre + 0.044715 * pre * pre * pre)
    tangent = jnp.tanh(inner)
    value = 0.5 * pre * (1.0 + tangent)
    slope = 0.5 * (1.0 + tangent) + 0.5 * pre * (1.0 - tangent * tangent) * ROOT_TWO_PI * (
        1.0 + 3.0 * 0.044715 * pre * pre
    )
    return (value, slope)


def ordered_sum(held, slots, me, size):
    total = jnp.zeros(held.shape, jnp.float32)
    for device in range(size):
        piece = jnp.where(me == device, held[...], 0.0)
        for step in range(1, size):
            piece = piece + jnp.where(lax.rem(me + size - step, size) == device, slots[step - 1], 0.0)
        total = total + piece
    return total


def sum_kernel(
    dp, tensor, late_ref, early_ref, out_ref, late_slots, all_slots, held_ref, send_a, recv_a, send_b, recv_b
):
    axes = (("tensor", tensor), ("dp", dp))
    barrier = pltpu.get_barrier_semaphore()
    for name, size in axes:
        me = lax.axis_index(name)
        for step in range(1, size):
            pl.semaphore_signal(
                barrier, inc=1, device_id={name: lax.rem(me + step, size)}, device_id_type=MESH
            )
    pl.semaphore_wait(barrier, dp + tensor - 2)

    def exchange(name, size, source, slots, send, receive):
        me = lax.axis_index(name)
        copies = []
        for step in range(1, size):
            copy = pltpu.make_async_remote_copy(
                src_ref=source,
                dst_ref=slots.at[step - 1],
                send_sem=send.at[step - 1],
                recv_sem=receive.at[step - 1],
                device_id={name: lax.rem(me + step, size)},
                device_id_type=MESH,
            )
            copy.start()
            copies.append(copy)
        for copy in copies:
            copy.wait()
        return ordered_sum(source, slots, me, size)

    rows = late_ref.shape[0]
    held_ref[rows:, :] = early_ref[...]
    held_ref[:rows, :] = exchange("tensor", tensor, late_ref, late_slots, send_a, recv_a)
    out_ref[...] = exchange("dp", dp, held_ref, all_slots, send_b, recv_b)


def small_sum(late, early, dp, tensor):
    rows = late.shape[0] + early.shape[0]
    vmem = pl.BlockSpec(memory_space=pltpu.VMEM)
    return pl.pallas_call(
        functools.partial(sum_kernel, dp, tensor),
        out_shape=jax.ShapeDtypeStruct((rows, 128), jnp.float32),
        in_specs=[vmem, vmem],
        out_specs=vmem,
        scratch_shapes=[
            pltpu.VMEM((tensor - 1, *late.shape), jnp.float32),
            pltpu.VMEM((dp - 1, rows, 128), jnp.float32),
            pltpu.VMEM((rows, 128), jnp.float32),
            pltpu.SemaphoreType.DMA((tensor - 1,)),
            pltpu.SemaphoreType.DMA((tensor - 1,)),
            pltpu.SemaphoreType.DMA((dp - 1,)),
            pltpu.SemaphoreType.DMA((dp - 1,)),
        ],
        compiler_params=pltpu.CompilerParams(collective_id=1, has_side_effects=True),
        name="small_sum",
    )(late, early)


def lanes_of(*parts):
    made = jnp.concatenate([part.reshape(-1, 128) for part in parts], axis=0)
    return jnp.pad(made, ((0, -made.shape[0] % 8), (0, 0)))


LOG2E = 1.4426950408889634
BLOCK = 256


def attention_tasks(segments, place, slots):
    length = segments.shape[0]
    begins = jnp.sum(
        (segments[None, :] < jnp.arange(1, 4, dtype=jnp.int32)[:, None]).astype(jnp.int32), axis=1
    )
    start = jnp.zeros_like(segments)
    for number in range(1, 4):
        start = jnp.where(segments == number, begins[number - 1], start)
    blocks = length // BLOCK
    first = start.reshape(blocks, BLOCK)[:, 0] // BLOCK
    entry = jnp.arange(blocks * blocks, dtype=jnp.int32)
    query, key = entry // blocks, lax.rem(entry, blocks)
    lowest = jnp.repeat(first, blocks)
    valid = (key <= query) & (key >= lowest)
    ahead = jnp.sum((valid[None, :] & (entry[None, :] < entry[:, None])).astype(jnp.int32), axis=1)
    count = jnp.sum(valid.astype(jnp.int32))
    room = blocks * (blocks + 1) // 2 + 4
    task = jnp.arange(room, dtype=jnp.int32)
    chosen = valid[None, :] & (ahead[None, :] == task[:, None])
    pick = lambda values: jnp.sum(jnp.where(chosen, values[None, :], 0), axis=1)
    per = blocks // slots
    lies = lambda block: lax.rem(place - block // per + slots, slots) * per + lax.rem(block, per)
    rows = [pick(query), jnp.where(task < count, pick(key), 1)]
    rows += [lies(rows[0]), lies(rows[1]), lies(lax.rem(task, blocks)), jnp.full_like(task, count)]
    return start, jnp.stack(rows)


def natural(block):
    return pl.ds(pl.multiple_of(block * BLOCK, BLOCK), BLOCK)


def head_rows(values, head):
    row = lax.broadcasted_iota(jnp.int32, values.shape, 0)
    return jnp.where(row // HD == head, values, jnp.zeros_like(values))


def head_lanes(values, head):
    lane = lax.broadcasted_iota(jnp.int32, values.shape, 1)
    return jnp.where(lane // HD == head, values, jnp.zeros_like(values))


def allowed_tile(start_row, key_block, query_block):
    key_index = lax.broadcasted_iota(jnp.int32, (BLOCK, BLOCK), 0)
    query_index = lax.broadcasted_iota(jnp.int32, (1, BLOCK), 1)
    last = (query_block - key_block) * BLOCK + query_index
    return (key_index <= last) & (key_index >= start_row - key_block * BLOCK)


def pipelined(tasks, stage_a, stage_b, stage_c):
    pairs = (tasks[5, 0] + 1) // 2
    stage_a(0, 0)

    @pl.loop(0, pairs)
    def _(pair):
        for half in range(2):
            task = 2 * pair + half
            stage_a(task + 1, 1 - half)
            stage_c(jnp.maximum(task - 1, 0), 1 - half)
            stage_b(task, half)

    stage_c(2 * pairs - 1, 1)


def forward_kernel(
    tasks, start_ref, q_ref, k_ref, v_ref, out_ref, lse_ref,
    qt_ref, vt_ref, acc_ref, peak_ref, total_ref, *slots,
):
    blocks = k_ref.shape[0] // BLOCK
    scores_ref, probs_ref, shrink_ref = slots[0:2], slots[2:4], slots[4:6]
    scale = HD**-0.5 * LOG2E
    peak_ref[...] = jnp.full_like(peak_ref, NEGATIVE)
    total_ref[...] = jnp.zeros_like(total_ref)
    acc_ref[...] = jnp.zeros_like(acc_ref)
    probs_ref[1][...] = jnp.zeros_like(probs_ref[1])
    shrink_ref[1][...] = jnp.ones_like(shrink_ref[1])

    @pl.loop(0, blocks)
    def _(b):
        at, held = natural(b), natural(tasks[4, b])
        vt_ref[:, at] = v_ref[held, :].T
        query = q_ref[held, :].T
        for head in range(2):
            qt_ref[head, :, at] = head_rows(query, head)

    def stage_a(task, slot):
        key = k_ref[natural(tasks[3, task]), :]
        for head in range(2):
            scores_ref[slot][head] = jnp.dot(
                key, qt_ref[head, :, natural(tasks[0, task])], preferred_element_type=jnp.float32
            )

    def stage_b(task, slot):
        i, j = tasks[0, task], tasks[1, task]
        at = natural(i)
        allowed = allowed_tile(start_ref[:, at], j, i)
        for head in range(2):
            row = slice(head, head + 1)
            scores = jnp.where(allowed, scores_ref[slot][head], NEGATIVE)
            peak = peak_ref[row, at]
            top = jnp.maximum(peak, jnp.max(scores, axis=0, keepdims=True))
            probs = jnp.exp2(scores * scale - top * scale)
            shrink = jnp.exp2((peak - top) * scale)
            peak_ref[row, at] = top
            total_ref[row, at] = total_ref[row, at] * shrink + jnp.sum(probs, axis=0, keepdims=True)
            shrink_ref[slot][row, :] = shrink
            probs_ref[slot][head] = probs.astype(jnp.bfloat16)

    def stage_c(task, slot):
        at, keys = natural(tasks[0, task]), natural(tasks[1, task])
        for head in range(2):
            rows = slice(head * HD, (head + 1) * HD)
            acc_ref[rows, at] = acc_ref[rows, at] * shrink_ref[slot][head : head + 1, :] + jnp.dot(
                vt_ref[rows, keys], probs_ref[slot][head], preferred_element_type=jnp.float32
            )

    pipelined(tasks, stage_a, stage_b, stage_c)

    @pl.loop(0, blocks)
    def _(b):
        at = natural(b)
        rows = [
            acc_ref[head * HD : (head + 1) * HD, at] / total_ref[head : head + 1, at]
            for head in range(2)
        ]
        out_ref[natural(tasks[4, b]), :] = jnp.concatenate(rows, axis=0).T.astype(jnp.bfloat16)
        lse_ref[0, :, at] = peak_ref[:, at] * scale + jnp.log2(total_ref[:, at])


def attention_forward(tasks, start, query, key, value):
    length, cols = query.shape
    width = 2 * HD
    pairs = cols // width
    whole = pl.BlockSpec((length, width), lambda p, b: (0, p))
    square = (2, BLOCK, BLOCK)
    return pl.pallas_call(
        forward_kernel,
        out_shape=(
            jax.ShapeDtypeStruct((length, cols), jnp.bfloat16),
            jax.ShapeDtypeStruct((pairs, 2, length), jnp.float32),
        ),
        grid_spec=pltpu.PrefetchScalarGridSpec(
            num_scalar_prefetch=1,
            grid=(pairs,),
            in_specs=[pl.BlockSpec((1, length), lambda p, b: (0, 0)), whole, whole, whole],
            out_specs=(whole, pl.BlockSpec((1, 2, length), lambda p, b: (p, 0, 0))),
            scratch_shapes=[
                pltpu.VMEM((2, width, length), jnp.bfloat16),
                pltpu.VMEM((width, length), jnp.bfloat16),
                pltpu.VMEM((width, length), jnp.float32),
                pltpu.VMEM((2, length), jnp.float32),
                pltpu.VMEM((2, length), jnp.float32),
            ]
            + [pltpu.VMEM(square, jnp.float32)] * 2
            + [pltpu.VMEM(square, jnp.bfloat16)] * 2
            + [pltpu.VMEM((2, BLOCK), jnp.float32)] * 2,
        ),
        compiler_params=pltpu.CompilerParams(dimension_semantics=("arbitrary",)),
        cost_estimate=pl.CostEstimate(
            flops=16 * 10**9, bytes_accessed=4 * 2 * length * cols, transcendentals=0
        ),
        name="attention_forward",
    )(tasks, start.reshape(1, length), query, key, value)


def turn(values, cosine, sine, sign):
    lane = lax.broadcasted_iota(jnp.int32, values.shape, 1)
    half = ROT // 2
    right = pltpu.roll(values, half, 1)
    left = pltpu.roll(values, values.shape[1] - half, 1)
    mixed = jnp.where(lane % HD < half, -left, right)
    return values * cosine + (sign * mixed) * sine


def backward_kernel(
    carried, tasks, start_ref, cos_ref, sin_ref, q_ref, k_ref, v_ref, out_ref, grad_ref, lse_ref, *refs
):
    dq_ref, dk_ref, dv_ref, bias_ref = refs[carried : carried + 4]
    qt_ref, gt_ref, kt_ref, dqt_ref, dka_ref, dva_ref, delta_ref, *slots = refs[carried + 4 :]
    blocks = q_ref.shape[0] // BLOCK
    scores_ref, back_ref, probs_ref, sgrad_ref = slots[0:2], slots[2:4], slots[4:6], slots[6:8]
    scale = HD**-0.5 * LOG2E
    dqt_ref[...] = jnp.zeros_like(dqt_ref)
    dka_ref[...] = jnp.zeros_like(dka_ref)
    dva_ref[...] = jnp.zeros_like(dva_ref)
    bias_ref[...] = jnp.zeros_like(bias_ref)
    probs_ref[1][...] = jnp.zeros_like(probs_ref[1])
    sgrad_ref[1][...] = jnp.zeros_like(sgrad_ref[1])

    @pl.loop(0, blocks)
    def _(b):
        at, held = natural(b), natural(tasks[4, b])
        grad = grad_ref[held, :]
        query_t, grad_t = q_ref[held, :].T, grad.T
        kt_ref[:, at] = k_ref[held, :].T
        both = (grad.astype(jnp.float32) * out_ref[held, :].astype(jnp.float32)).T
        for head in range(2):
            qt_ref[head, :, at] = head_rows(query_t, head)
            gt_ref[head, :, at] = head_rows(grad_t, head)
            delta_ref[head : head + 1, at] = jnp.sum(
                both[head * HD : (head + 1) * HD], axis=0, keepdims=True
            )

    def stage_a(task, slot):
        at, keys = natural(tasks[0, task]), natural(tasks[3, task])
        key, value = k_ref[keys, :], v_ref[keys, :]
        for head in range(2):
            scores_ref[slot][head] = jnp.dot(
                key, qt_ref[head, :, at], preferred_element_type=jnp.float32
            )
            back_ref[slot][head] = jnp.dot(
                value, gt_ref[head, :, at], preferred_element_type=jnp.float32
            )

    def stage_b(task, slot):
        i, j = tasks[0, task], tasks[1, task]
        at = natural(i)
        allowed = allowed_tile(start_ref[:, at], j, i)
        for head in range(2):
            probs = jnp.exp2(scores_ref[slot][head] * scale - lse_ref[0, head : head + 1, at])
            probs = jnp.where(allowed, probs, 0.0)
            probs_ref[slot][head] = probs.astype(jnp.bfloat16)
            sgrad_ref[slot][head] = (
                probs * (back_ref[slot][head] - delta_ref[head : head + 1, at])
            ).astype(jnp.bfloat16)

    def stage_c(task, slot):
        at, keys = natural(tasks[0, task]), natural(tasks[1, task])
        held = natural(tasks[2, task])
        query, grad = q_ref[held, :], grad_ref[held, :]
        for target, left, right in ((dva_ref, probs_ref, grad), (dka_ref, sgrad_ref, query)):
            target[keys, :] += sum(
                jnp.dot(
                    left[slot][head], head_lanes(right, head), preferred_element_type=jnp.float32
                )
                for head in range(2)
            )
        for head in range(2):
            rows = slice(head * HD, (head + 1) * HD)
            dqt_ref[rows, at] += jnp.dot(
                kt_ref[rows, keys], sgrad_ref[slot][head], preferred_element_type=jnp.float32
            )

    pipelined(tasks, stage_a, stage_b, stage_c)

    @pl.loop(0, blocks)
    def _(b):
        at, held = natural(b), natural(tasks[4, b])
        cosine, sine = cos_ref[at, :], sin_ref[at, :]
        grads = (
            turn(dqt_ref[:, at].T * HD**-0.5, cosine, sine, -1.0),
            turn(dka_ref[at, :] * HD**-0.5, cosine, sine, -1.0),
            dva_ref[at, :],
        )
        for part, (out, grad) in enumerate(zip((dq_ref, dk_ref, dv_ref), grads)):
            out[held, :] = grad.astype(jnp.bfloat16)
            bias_ref[part : part + 1, :] += jnp.sum(grad, axis=0, keepdims=True)


def attention_backward(
    part, tasks, start, cosine, sine, query, key, value, attended, grad, lse, before
):
    length, cols = query.shape
    width = 2 * HD
    first, pairs = part
    whole = pl.BlockSpec((length, width), lambda p, b: (0, first + p))
    table = pl.BlockSpec((length, width), lambda p, b: (0, 0))
    shape = jax.ShapeDtypeStruct((length, cols), jnp.bfloat16)
    square = (2, BLOCK, BLOCK)
    carried = len(before)
    return pl.pallas_call(
        functools.partial(backward_kernel, carried),
        out_shape=(shape, shape, shape, jax.ShapeDtypeStruct((3, cols), jnp.float32)),
        grid_spec=pltpu.PrefetchScalarGridSpec(
            num_scalar_prefetch=1,
            grid=(pairs,),
            in_specs=[
                pl.BlockSpec((1, length), lambda p, b: (0, 0)),
                table,
                table,
                whole,
                whole,
                whole,
                whole,
                whole,
                pl.BlockSpec((1, 2, length), lambda p, b: (first + p, 0, 0)),
            ]
            + [pl.BlockSpec(memory_space=pl.ANY)] * carried,
            out_specs=(whole, whole, whole, pl.BlockSpec((3, width), lambda p, b: (0, first + p))),
            scratch_shapes=[
                pltpu.VMEM((2, width, length), jnp.bfloat16),
                pltpu.VMEM((2, width, length), jnp.bfloat16),
                pltpu.VMEM((width, length), jnp.bfloat16),
                pltpu.VMEM((width, length), jnp.float32),
                pltpu.VMEM((length, width), jnp.float32),
                pltpu.VMEM((length, width), jnp.float32),
                pltpu.VMEM((2, length), jnp.float32),
            ]
            + [pltpu.VMEM(square, jnp.float32)] * 4
            + [pltpu.VMEM(square, jnp.bfloat16)] * 4,
        ),
        input_output_aliases={10 + i: i for i in range(carried)},
        compiler_params=pltpu.CompilerParams(dimension_semantics=("arbitrary",)),
        cost_estimate=pl.CostEstimate(
            flops=10**10 * pairs, bytes_accessed=8 * 2 * length * width * pairs, transcendentals=0
        ),
        name="attention_backward",
    )(tasks, start.reshape(1, length), cosine, sine, query, key, value, attended, grad, lse, *before)


def rotary_tables(segments, start):
    length = segments.shape[0]
    place = (jnp.arange(length, dtype=jnp.int32) - start).astype(jnp.float32)
    freq = 10000.0 ** (-(2.0 * jnp.arange(ROT // 2, dtype=jnp.float32)) / ROT)
    lane = jnp.arange(2 * HD, dtype=jnp.int32) % HD
    angle = place[:, None] * jnp.tile(freq, 2 * HD // (ROT // 2))[None, :]
    turned = (lane < ROT)[None, :]
    return jnp.where(turned, jnp.cos(angle), 1.0), jnp.where(turned, jnp.sin(angle), 0.0)


TILE = 1024


def dot_nt(left, right):
    return lax.dot_general(left, right, (((1,), (1,)), ((), ())), preferred_element_type=jnp.float32)


def dot_nn(left, right):
    return jnp.dot(left, right, preferred_element_type=jnp.float32)


def lanes(index, size):
    return pl.ds(pl.multiple_of(index * size, size), size)


def chunk_kernel(
    at, hidden_ref, qkv_ref, bias_ref, cos_ref, sin_ref, up_ref, up_bias_ref, down_ref, *refs
):
    q_ref, k_ref, v_ref, act_ref, slope_ref, all_ref, part_ref = refs[-7:]
    step = pl.program_id(0)
    width = 2 * HD

    @pl.when(step == 0)
    def _():
        all_ref[...] = hidden_ref[...]
        part_ref[...] = jnp.zeros_like(part_ref)
        for part, out in enumerate((q_ref, k_ref, v_ref)):
            made = dot_nn(hidden_ref[...], qkv_ref[part]) + bias_ref[part : part + 1, :]
            for pair in range(made.shape[1] // width):
                where = slice(pair * width, (pair + 1) * width)
                piece = made[:, where]
                if part < 2:
                    piece = turn(piece, cos_ref[...], sin_ref[...], 1.0)
                out[:, where] = piece.astype(jnp.bfloat16)

    @pl.when(step > 0)
    def _():
        small = 256

        @pl.loop(0, up_ref.shape[1] // small)
        def _(n):
            where = lanes(n, small)
            value, slope = gelu_pair(dot_nn(hidden_ref[...], up_ref[:, where]) + up_bias_ref[:, where])
            act_ref[:, where] = value.astype(jnp.bfloat16)
            slope_ref[:, where] = slope.astype(jnp.bfloat16)

        @pl.loop(0, part_ref.shape[1] // (2 * small))
        def _(n):
            where = lanes(n, 2 * small)
            part_ref[:, where] += dot_nn(act_ref[...], down_ref[:, where])


def chunk_forward(slot, slots, hidden, weight, bias, cosine, sine, up_weight, up_bias, down_weight, before):
    rows, depth = hidden.shape
    cols, units = weight.shape[2], up_weight.shape[1]
    width = 2 * HD
    tile = min(TILE, units)
    tiles = units // tile
    length = slots * rows
    made = [jax.ShapeDtypeStruct((length, n), jnp.bfloat16) for n in (cols, cols, cols, units, units, depth)]
    made.append(jax.ShapeDtypeStruct((length, depth), jnp.float32))
    once = lambda shape: pl.BlockSpec(
        shape, lambda s, at: (0,) * len(shape), pipeline_mode=pl.Buffered(1)
    )
    unit = lambda s: jnp.maximum(s - 1, 0)
    row = lambda shape: pl.BlockSpec(shape, lambda s, at: (at[0], 0))
    out = row((rows, cols))
    wide = pl.BlockSpec((rows, tile), lambda s, at: (at[0], unit(s)))
    return pl.pallas_call(
        chunk_kernel,
        out_shape=made,
        grid_spec=pltpu.PrefetchScalarGridSpec(
            num_scalar_prefetch=1,
            grid=(1 + tiles,),
            in_specs=[
                once((rows, depth)),
                once((3, depth, cols)),
                once((3, cols)),
                once((rows, width)),
                once((rows, width)),
                pl.BlockSpec((depth, tile), lambda s, at: (0, unit(s))),
                pl.BlockSpec((1, tile), lambda s, at: (0, unit(s))),
                pl.BlockSpec((tile, depth), lambda s, at: (unit(s), 0)),
            ]
            + [pl.BlockSpec(memory_space=pl.ANY)] * len(before),
            out_specs=[out, out, out, wide, wide, row((rows, depth)), row((rows, depth))],
        ),
        input_output_aliases={9 + i: i for i in range(len(before))},
        compiler_params=pltpu.CompilerParams(dimension_semantics=("arbitrary",)),
        cost_estimate=pl.CostEstimate(
            flops=2 * rows * depth * (3 * cols + 2 * units),
            bytes_accessed=2 * depth * (4 * rows + 3 * cols + 2 * units) + 2 * rows * (3 * cols + 2 * units),
            transcendentals=rows * units,
        ),
        name="chunk_forward",
    )(
        jnp.full((1,), slot, jnp.int32), hidden, weight, bias, cosine, sine,
        up_weight, up_bias.reshape(1, units), down_weight, *before,
    )


def branch_kernel(at, part_ref, left_ref, right_ref, out_ref):
    out_ref[...] = (part_ref[...] + dot_nn(left_ref[...], right_ref[...])).astype(jnp.bfloat16)


def branch_part(slot, rows, part, attended, out_weight):
    cols, depth = out_weight.shape
    return pl.pallas_call(
        branch_kernel,
        out_shape=jax.ShapeDtypeStruct((rows, depth), jnp.bfloat16),
        grid_spec=pltpu.PrefetchScalarGridSpec(
            num_scalar_prefetch=1,
            grid=(2,),
            in_specs=[
                pl.BlockSpec((rows, depth // 2), lambda n, at: (at[0], n)),
                pl.BlockSpec((rows, cols), lambda n, at: (at[0], 0)),
                pl.BlockSpec((cols, depth // 2), lambda n, at: (0, n)),
            ],
            out_specs=pl.BlockSpec((rows, depth // 2), lambda n, at: (0, n)),
        ),
        compiler_params=pltpu.CompilerParams(dimension_semantics=("arbitrary",)),
        cost_estimate=pl.CostEstimate(
            flops=2 * rows * cols * depth,
            bytes_accessed=6 * rows * depth + 2 * cols * (rows + depth),
            transcendentals=0,
        ),
        name="branch_part",
    )(slot, part, attended, out_weight)


def hidden_kernel(at, q_ref, k_ref, v_ref, act_ref, qkv_ref, up_ref, out_ref):
    total = dot_nt(act_ref[...], up_ref[...])
    for part, left in enumerate((q_ref, k_ref, v_ref)):
        total = total + dot_nt(left[...], qkv_ref[part])
    out_ref[...] = total.astype(jnp.bfloat16)


def hidden_part(slot, rows, parts, act_grad, qkv_weight, up_weight):
    depth, units = up_weight.shape
    cols = qkv_weight.shape[2]
    tile = min(TILE, depth)
    left = lambda n: pl.BlockSpec((rows, n), lambda s, at: (at[0], 0))
    return pl.pallas_call(
        hidden_kernel,
        out_shape=jax.ShapeDtypeStruct((rows, depth), jnp.bfloat16),
        grid_spec=pltpu.PrefetchScalarGridSpec(
            num_scalar_prefetch=1,
            grid=(depth // tile,),
            in_specs=[
                left(cols),
                left(cols),
                left(cols),
                left(units),
                pl.BlockSpec((3, tile, cols), lambda s, at: (0, s, 0)),
                pl.BlockSpec((tile, units), lambda s, at: (s, 0)),
            ],
            out_specs=pl.BlockSpec((rows, tile), lambda s, at: (0, s)),
        ),
        compiler_params=pltpu.CompilerParams(dimension_semantics=("arbitrary",)),
        cost_estimate=pl.CostEstimate(
            flops=2 * rows * depth * (3 * cols + units),
            bytes_accessed=2 * (rows + depth) * (3 * cols + units),
            transcendentals=0,
        ),
        name="hidden_part",
    )(slot, *parts, act_grad, qkv_weight, up_weight)


def chunk_back_kernel(
    at, left_a, right_a, left_b, right_b, down_ref, out_w_ref, slope_ref, *refs
):
    act_ref, attend_ref, all_ref, sum_ref = refs[-5:-1]
    held_ref = refs[-1]
    step, chunk = pl.program_id(0), pl.program_id(1)
    for number, (left, right) in enumerate(((left_a, right_a), (left_b, right_b))):

        @pl.when((step == 0) & (chunk == number))
        def _(number=number, left=left, right=right):
            held_ref[number] = left[...] + right[...]

    @pl.when(step == 0)
    def _():
        all_ref[...] = held_ref[chunk]
        attend_ref[...] = dot_nt(held_ref[chunk], out_w_ref[...]).astype(jnp.bfloat16)

    @pl.when(step > 0)
    def _():
        small = 512

        @pl.when(chunk == 0)
        def _():
            sum_ref[...] = jnp.zeros_like(sum_ref)

        @pl.loop(0, down_ref.shape[0] // small)
        def _(n):
            where = lanes(n, small)
            made = dot_nt(held_ref[chunk], down_ref[where, :]) * slope_ref[:, where].astype(jnp.float32)
            act_ref[:, where] = made.astype(jnp.bfloat16)
            sum_ref[:, where] += jnp.sum(made, axis=0, keepdims=True)


def chunk_backward(pair, slots, halves, down_weight, out_weight, slope, before):
    rows, depth = halves[0].shape
    units, cols = down_weight.shape[0], out_weight.shape[0]
    tile = min(TILE, units)
    length = slots * rows
    unit = lambda n: jnp.maximum(n - 1, 0)
    late = lambda n, r: jnp.where(n == 0, r, 1)
    half = pl.BlockSpec((rows, depth), lambda n, r, at: (0, 0), pipeline_mode=pl.Buffered(1))
    wide = pl.BlockSpec((rows, tile), lambda n, r, at: (at[jnp.where(n == 0, 0, r)], unit(n)))
    return pl.pallas_call(
        chunk_back_kernel,
        out_shape=(
            jax.ShapeDtypeStruct((length, units), jnp.bfloat16),
            jax.ShapeDtypeStruct((length, cols), jnp.bfloat16),
            jax.ShapeDtypeStruct((length, depth), jnp.bfloat16),
            jax.ShapeDtypeStruct((1, units), jnp.float32),
        ),
        grid_spec=pltpu.PrefetchScalarGridSpec(
            num_scalar_prefetch=1,
            grid=(1 + units // tile, 2),
            in_specs=[
                half,
                half,
                half,
                half,
                pl.BlockSpec((tile, depth), lambda n, r, at: (unit(n), 0)),
                pl.BlockSpec((cols, depth), lambda n, r, at: (0, 0), pipeline_mode=pl.Buffered(1)),
                wide,
            ]
            + [pl.BlockSpec(memory_space=pl.ANY)] * len(before),
            out_specs=(
                wide,
                pl.BlockSpec((rows, cols), lambda n, r, at: (at[late(n, r)], 0)),
                pl.BlockSpec((rows, depth), lambda n, r, at: (at[late(n, r)], 0)),
                pl.BlockSpec((1, tile), lambda n, r, at: (0, unit(n))),
            ),
            scratch_shapes=[pltpu.VMEM((2, rows, depth), jnp.bfloat16)],
        ),
        input_output_aliases={8 + i: i for i in range(len(before))},
        compiler_params=pltpu.CompilerParams(dimension_semantics=("arbitrary", "arbitrary")),
        cost_estimate=pl.CostEstimate(
            flops=4 * rows * depth * (units + cols),
            bytes_accessed=2 * depth * (8 * rows + units + cols) + 8 * rows * units,
            transcendentals=0,
        ),
        name="chunk_backward",
    )(jnp.array(pair, jnp.int32), *halves, down_weight, out_weight, slope, *before)


def finish_kernel(own, right, left, block_ref, grad_ref, gain_ref, out_ref, sum_ref):
    hidden_grad = (
        own[...].astype(jnp.float32) + right[...].astype(jnp.float32) + left[...].astype(jnp.float32)
    )
    normed, inv_scale = normalize(block_ref[...])

    @pl.when(pl.program_id(0) == 0)
    def _():
        sum_ref[...] = jnp.zeros_like(sum_ref)

    grad = grad_ref[...].astype(jnp.float32)
    sum_ref[0:1, :] += jnp.sum(hidden_grad * normed, axis=0, keepdims=True)
    sum_ref[1:2, :] += jnp.sum(hidden_grad, axis=0, keepdims=True)
    scaled = hidden_grad * gain_ref[...]
    inner = (
        scaled
        - jnp.mean(scaled, axis=-1, keepdims=True)
        - normed * jnp.mean(scaled * normed, axis=-1, keepdims=True)
    )
    out_ref[...] = (grad + inv_scale * inner).astype(jnp.bfloat16)


def finish(own, right, left, block_in, cotangent, ln_gain):
    rows, depth = own.shape
    step = min(128, rows)
    block = pl.BlockSpec((step, depth), lambda r: (r, 0))
    return pl.pallas_call(
        finish_kernel,
        out_shape=(
            jax.ShapeDtypeStruct((rows, depth), jnp.bfloat16),
            jax.ShapeDtypeStruct((2, depth), jnp.float32),
        ),
        grid=(rows // step,),
        in_specs=[block] * 5 + [pl.BlockSpec((1, depth), lambda r: (0, 0))],
        out_specs=(block, pl.BlockSpec((2, depth), lambda r: (0, 0))),
        compiler_params=pltpu.CompilerParams(dimension_semantics=("arbitrary",)),
        cost_estimate=pl.CostEstimate(
            flops=20 * rows * depth, bytes_accessed=12 * rows * depth, transcendentals=0
        ),
        name="finish",
    )(own, right, left, block_in, cotangent, ln_gain.reshape(1, depth))


def begin_kernel(block_ref, gain_ref, shift_ref, out_ref):
    normed, _ = normalize(block_ref[...])
    out_ref[...] = (normed * gain_ref[...] + shift_ref[...]).astype(jnp.bfloat16)


def begin(block_in, ln_gain, ln_bias):
    rows, depth = block_in.shape
    step = min(128, rows)
    block = pl.BlockSpec((step, depth), lambda r: (r, 0))
    row = pl.BlockSpec((1, depth), lambda r: (0, 0))
    return pl.pallas_call(
        begin_kernel,
        out_shape=jax.ShapeDtypeStruct((rows, depth), jnp.bfloat16),
        grid=(rows // step,),
        in_specs=[block, row, row],
        out_specs=block,
        compiler_params=pltpu.CompilerParams(dimension_semantics=("arbitrary",)),
        cost_estimate=pl.CostEstimate(
            flops=10 * rows * depth, bytes_accessed=4 * rows * depth, transcendentals=0
        ),
        name="begin",
    )(block_in, ln_gain.reshape(1, depth), ln_bias.reshape(1, depth))


def line(size, right, step):
    return [(i, i + 1 if right else i - 1) for i in step if 0 <= (i + 1 if right else i - 1) < size]


def ring_gather(own, size):
    pairs = [(i, (i + 1) % size) for i in range(size)]
    slots = [own]
    for _ in range(1, size):
        slots.append(lax.ppermute(slots[-1], "tensor", pairs))
    return slots


def line_gather(own, size):
    from_left, from_right = [own], [own]
    for step in range(1, size):
        from_left.append(
            lax.ppermute(from_left[-1], "tensor", line(size, True, range(step - 1, size)))
        )
        from_right.append(
            lax.ppermute(from_right[-1], "tensor", line(size, False, range(size - step + 1)))
        )
    return from_left, from_right


def slot_of(place, size, turn_number):
    return jnp.where(2 * place < size, turn_number, (size - turn_number) % size).reshape(1)


def line_scatter(turns, place, size):
    low = 2 * place < size
    right = left = None
    for step in range(1, size):
        go_right = go_left = turns[step]
        if 2 * step > size:
            go_right = jnp.where(low, turns[step], turns[size - step])
            go_left = jnp.where(low, turns[size - step], turns[step])
        if step > 1:
            go_right, go_left = go_right + right, go_left + left
        right = lax.ppermute(go_right, "tensor", line(size, True, range(step)))
        left = lax.ppermute(go_left, "tensor", line(size, False, range(size - step, size)))
    return right, left


def turns_of(place, size, make):
    made = {}
    for number in [*range(1, size), 0]:
        made[number] = make(slot_of(place, size, number))
    return made


def slot_pairs(size):
    half = size // 2
    return [(0, half)] + [(half - step, half + step) for step in range(1, half)]


def layer(
    sizes,
    block_in,
    ln_gain,
    ln_bias,
    qkv_weight,
    qkv_bias,
    out_weight,
    out_bias,
    up_weight,
    up_bias,
    down_weight,
    down_bias,
    segments,
    cotangent,
):
    dp, tensor = sizes
    depth = block_in.shape[1]
    units = up_weight.shape[1]
    cols = qkv_weight.shape[2]
    contract_rows = (((0,), (0,)), ((), ()))
    rows = block_in.shape[0]
    place = lax.axis_index("tensor")
    hidden_own = begin(block_in, ln_gain, ln_bias)
    chunks = ring_gather(hidden_own, tensor)
    start, tasks = attention_tasks(segments, place, tensor)
    cosine, sine = rotary_tables(segments, start)
    made = []
    for slot, chunk in enumerate(chunks):
        offset = lax.rem(place - slot + tensor, tensor) * rows
        turned = [lax.dynamic_slice_in_dim(table, offset, rows, 0) for table in (cosine, sine)]
        made = chunk_forward(slot, tensor, chunk, qkv_weight, qkv_bias, *turned, up_weight, up_bias, down_weight, made)
    query, key, value, act, slope, hidden, down_part = made
    grad_own, _ = lax.optimization_barrier((cotangent, chunks[-1]))
    from_left, from_right = line_gather(grad_own, tensor)
    attended, log_sums = attention_forward(tasks, start, query, key, value)
    branch = turns_of(place, tensor, lambda slot: branch_part(slot, rows, down_part, attended, out_weight))
    right, left = line_scatter(branch, place, tensor)
    wide = [part.astype(jnp.float32) for part in (branch[0], right, left)]
    block_out = (
        block_in.astype(jnp.float32) + (wide[0] + wide[1] + wide[2]) + out_bias + down_bias
    ).astype(jnp.bfloat16)
    bias_sum = jnp.sum(cotangent.astype(jnp.float32), axis=0)
    made, up_bias_parts = [], []
    nothing = jnp.zeros_like(cotangent)
    for pair in slot_pairs(tensor):
        halves = []
        for slot in pair:
            halves += [from_left[slot], from_right[tensor - slot] if slot else nothing]
        *made, sums = chunk_backward(pair, tensor, halves, down_weight, out_weight, slope, made)
        up_bias_parts.append(sums)
    act_grad, attended_grad, grad_out = made
    up_bias_local = sum(up_bias_parts)
    back = []
    pairs = cols // (2 * HD)
    for half in range(2):
        back = attention_backward(
            (half * (pairs // 2), pairs // 2),
            tasks, start, cosine, sine, query, key, value, attended, attended_grad, log_sums, back,
        )
    *parts, qkv_bias_local = back
    hidden_turns = turns_of(place, tensor, lambda slot: hidden_part(slot, rows, parts, act_grad, qkv_weight, up_weight))
    right, left = line_scatter(hidden_turns, place, tensor)
    cols_grad = jnp.stack(
        [
            lax.dot_general(one, two, contract_rows, preferred_element_type=jnp.float32).astype(
                jnp.bfloat16
            )
            for one, two in [(hidden, part) for part in parts] + [(grad_out, attended)]
        ]
    )
    down_grad = lax.dot_general(act, grad_out, contract_rows, preferred_element_type=jnp.float32).astype(jnp.bfloat16)
    up_grad = lax.dot_general(hidden, act_grad, contract_rows, preferred_element_type=jnp.float32).astype(jnp.bfloat16)
    cols_share = lax.psum_scatter(
        cols_grad, "dp", scatter_dimension=1, tiled=True
    ).astype(jnp.float32)
    down_share = lax.psum_scatter(
        down_grad, "dp", scatter_dimension=1, tiled=True
    ).astype(jnp.float32)
    up_share = lax.psum_scatter(up_grad, "dp", scatter_dimension=0, tiled=True).astype(jnp.float32)
    qkv_share, out_share = cols_share[:3], cols_share[3].T
    input_grad, norm_sums = finish(
        hidden_turns[0], right, left, block_in, cotangent, ln_gain
    )
    late = lanes_of(norm_sums, bias_sum)
    sums = small_sum(late, lanes_of(qkv_bias_local, up_bias_local), dp, tensor)
    gain_grad, shift_grad, bias_total = sums[: 3 * depth // 128].reshape(3, depth)
    early, qkv_rows = sums[late.shape[0] :], 3 * cols // 128
    qkv_bias_grad = early[:qkv_rows].reshape(3, cols)
    up_bias_grad = early[qkv_rows : qkv_rows + units // 128].reshape(units)
    return (
        block_out,
        input_grad,
        gain_grad,
        shift_grad,
        qkv_share,
        qkv_bias_grad,
        out_share,
        bias_total,
        up_share,
        up_bias_grad,
        down_share,
        bias_total,
    )


def local(sizes, *arrays):
    return layer(sizes, *arrays)


def solution(mesh):
    return jax.shard_map(
        functools.partial(local, (mesh.shape["dp"], mesh.shape["tensor"])),
        mesh=mesh,
        in_specs=(
            P(("dp", "tensor"), None),
            P(),
            P(),
            P(None, None, "tensor"),
            P(None, "tensor"),
            P("tensor", None),
            P(),
            P(None, "tensor"),
            P("tensor"),
            P("tensor", None),
            P(),
            P("dp"),
            P(("dp", "tensor"), None),
        ),
        out_specs=(
            P(("dp", "tensor"), None),
            P(("dp", "tensor"), None),
            P(),
            P(),
            P(None, "dp", "tensor"),
            P(None, "tensor"),
            P("tensor", "dp"),
            P(),
            P("dp", "tensor"),
            P("tensor"),
            P("tensor", "dp"),
            P(),
        ),
        check_vma=False,
    )
```
